32 devices in a mesh: ka: 16 (over z, x, core), sp: 2 (over y).
Axes of the slice: x: 2, y: 2, z: 4, core: 2. Of those that a mesh axis runs over, the one named last changes fastest.
Arguments:
- bloch_index: int32 [16, 2], P('ka'), may hold values from 0 to 63
- material: int32 [32, 64, 128], P('sp'), may hold values from 0 to 2
- permittivity: float32 [3], replicated, may hold values from 1 to 12
- absorption_peak: float32 [1], replicated, may hold values from 0.25 to 2
- source_sheet: float32 [16, 2, 32, 64], P('ka', None, 'sp'), may hold values from -6 to 6
- waveform: float32 [10], replicated, may hold values from -6 to 6
- electric_in: bfloat16 [16, 6, 32, 64, 128], P('ka', None, 'sp'), may hold values from -12 to 12
- magnetic_in: bfloat16 [16, 6, 32, 64, 128], P('ka', None, 'sp'), may hold values from -12 to 12
Outputs:
- electric_out: float32 [16, 6, 32, 64, 128], P('ka', None, 'sp')
- magnetic_out: float32 [16, 6, 32, 64, 128], P('ka', None, 'sp')
- reflected: float32 [16, 2], P('ka')
- reflected_mean: float32 [2], replicated
The draws below stay inside these ranges and needn't reach their ends.
All inputs are finite; a program needn't handle non-finite values.
Results may differ from the reference program's by a relative error of at most 0.0003.
Values sent between devices are 32-bit elements; how exact they have to be, the bound alone decides.
A program may use at most 64 MiB of HBM per device.

```python
import math
import jax
import jax.numpy as jnp
from jax import lax

NY = 64
NZ = 128
PML = 16
STEPS = 10
INTERVAL = 5
NSNAP = 2
MPHASE = 64
NMAT = 3
K = 16
NX = 32


def start_field(key, salt):
    key = jax.random.fold_in(key, salt)
    level_key, phase_key, noise_key, common_key = jax.random.split(key, 4)
    level = jax.random.uniform(level_key, (K, 1, 1, 1, 1), jnp.float32, -1.0, 1.0)
    amplitude = jnp.exp(0.6931472 * level)
    phase = jax.random.uniform(phase_key, (K, 1, 1, 1, 1), jnp.float32, 0.0, 6.2831853)
    across = jnp.arange(NX, dtype=jnp.float32).reshape(1, 1, NX, 1, 1)
    profile = 1.0 + 0.6 * jnp.sin(6.2831853 * across / NX + phase)
    full_shape = (K, 6, NX, NY, NZ)
    rough = jnp.clip(jax.random.normal(noise_key, full_shape, jnp.float32), -3.5, 3.5)
    return (amplitude * profile * rough).astype(jnp.bfloat16)


def draw_electric_in(key, part):
    return start_field(key, 11)


def draw_magnetic_in(key, part):
    return start_field(key, 23)


def set_ends(values, rng, low, top_value):
    longest = values.shape.index(max(values.shape))
    spots = []
    for shift in (0, 1):
        where = [jax.random.randint(jax.random.fold_in(rng, axis), (), 0, length) for axis, length in enumerate(values.shape)]
        where[longest] = (where[longest] + shift) % values.shape[longest]
        spots.append(tuple(where))
    return values.at[spots[0]].set(low).at[spots[1]].set(top_value)


def block_scale(rng, dims, cuts, low, largest):
    gain = 1.0
    for position, blocks in cuts:
        heights = jax.random.uniform(jax.random.fold_in(jax.random.fold_in(rng, 6), position), (blocks,), jnp.float32, low / len(cuts), largest / len(cuts))
        gain = gain * jnp.repeat(jnp.exp(heights), dims[position] // blocks).reshape((-1,) + (1,) * (len(dims) - 1 - position))
    return gain


def normal_values(stream_key, extent, deviation, reach, shards=(), kind=jnp.bfloat16):
    values = deviation * jax.random.normal(stream_key, extent, jnp.float32)
    if shards:
        values = values * block_scale(stream_key, extent, shards, -0.22, 0.18)
    return jnp.clip(values, -reach, reach).astype(kind)


def setup_inputs(seed: int = 0) -> dict:
    keys = jax.random.split(jax.random.key(seed), 9)
    bloch_index = set_ends(jax.random.randint(keys[0], (K, 2), 0, MPHASE), jax.random.fold_in(keys[0], 1), 0, MPHASE - 1).astype(jnp.int32)
    material = set_ends(jax.random.randint(keys[1], (NX, NY, NZ), 0, NMAT), jax.random.fold_in(keys[1], 1), 0, NMAT - 1).astype(jnp.int32)
    permittivity = jnp.clip(jnp.exp(jax.random.uniform(keys[2], (NMAT,), jnp.float32, math.log(1.0), math.log(12.0))), 1.0, 12.0)
    absorption_peak = jnp.clip(jnp.exp(jax.random.uniform(keys[3], (1,), jnp.float32, math.log(0.25), math.log(2.0))), 0.25, 2.0)
    source_sheet = normal_values(keys[4], (K, 2, NX, NY), 1.0, 6.0, ((0, 16), (2, 2)), jnp.float32)
    waveform = normal_values(keys[5], (STEPS,), 1.0, 6.0, (), jnp.float32)
    electric_in = draw_electric_in(jax.random.fold_in(keys[8], 71), 0)
    magnetic_in = draw_magnetic_in(jax.random.fold_in(keys[8], 71), 0)
    return dict(bloch_index=bloch_index, material=material, permittivity=permittivity, absorption_peak=absorption_peak, source_sheet=source_sheet, waveform=waveform, electric_in=electric_in, magnetic_in=magnetic_in)


TIME_STEP = 0.5


def rotate(couple, cosine, sine):
    return (couple[0] * cosine - couple[1] * sine, couple[0] * sine + couple[1] * cosine)


def subtract(left, right):
    return (left[0] - right[0], left[1] - right[1])


def slice_along(couple, begin_at, end_at, along):
    return tuple(lax.slice_in_dim(values, begin_at, end_at, axis=along) for values in couple)


def attach(front, back, along):
    return tuple(jnp.concatenate([first_part, second_part], axis=along) for first_part, second_part in zip(front, back))


def above_cell(couple, beyond, along):
    length = couple[0].shape[along]
    return attach(slice_along(couple, 1, length, along), beyond, along)


def below_cell(couple, beyond, along):
    length = couple[0].shape[along]
    return attach(beyond, slice_along(couple, 0, length - 1, along), along)


def forward_wrap(couple, along, cosine, sine):
    beyond = rotate(slice_along(couple, 0, 1, along), cosine, sine)
    return subtract(above_cell(couple, beyond, along), couple)


def backward_wrap(couple, along, cosine, sine):
    length = couple[0].shape[along]
    beyond = rotate(slice_along(couple, length - 1, length, along), cosine, -sine)
    return subtract(couple, below_cell(couple, beyond, along))


def forward_open(couple):
    along = couple[0].ndim - 1
    beyond = tuple(jnp.zeros_like(values) for values in slice_along(couple, 0, 1, along))
    return subtract(above_cell(couple, beyond, along), couple)


def backward_open(couple):
    along = couple[0].ndim - 1
    beyond = tuple(jnp.zeros_like(values) for values in slice_along(couple, 0, 1, along))
    return subtract(couple, below_cell(couple, beyond, along))


def electric_curl(electric, beyond_y, beyond_z, cosine, sine):
    ex_part, ey_part, ez_part = electric
    across = ex_part[0].ndim - 3
    sideways = across + 1
    dx_ey = subtract(above_cell(ey_part, beyond_y, across), ey_part)
    dx_ez = subtract(above_cell(ez_part, beyond_z, across), ez_part)
    return (subtract(forward_wrap(ez_part, sideways, cosine, sine), forward_open(ey_part)),
            subtract(forward_open(ex_part), dx_ez),
            subtract(dx_ey, forward_wrap(ex_part, sideways, cosine, sine)))


def magnetic_curl(magnetic, behind_y, behind_z, cosine, sine):
    hx_part, hy_part, hz_part = magnetic
    across = hx_part[0].ndim - 3
    sideways = across + 1
    bx_hy = subtract(hy_part, below_cell(hy_part, behind_y, across))
    bx_hz = subtract(hz_part, below_cell(hz_part, behind_z, across))
    return (subtract(backward_wrap(hz_part, sideways, cosine, sine), backward_open(hy_part)),
            subtract(backward_open(hx_part), bx_hz),
            subtract(bx_hy, backward_wrap(hx_part, sideways, cosine, sine)))


def relax(couple, change, retain, factor):
    return (retain * couple[0] + factor * change[0], retain * couple[1] + factor * change[1])


def coefficients(material, permittivity, absorption_peak, depth):
    height = jnp.arange(depth, dtype=jnp.float32)
    low_depth = jnp.maximum(PML - height, 0.0) / PML
    high_depth = jnp.maximum(height - (depth - 1 - PML), 0.0) / PML
    conduct = absorption_peak[0] * (low_depth ** 3 + high_depth ** 3)
    half_mag = conduct * (0.5 * TIME_STEP)
    h_retain = (1.0 - half_mag) / (1.0 + half_mag)
    h_factor = -TIME_STEP / (1.0 + half_mag)
    relative = jnp.zeros(material.shape, jnp.float32)
    for level in range(NMAT):
        relative = relative + jnp.where(material == level, permittivity[level], 0.0)
    half_ele = conduct * (0.5 * TIME_STEP) / relative
    e_retain = (1.0 - half_ele) / (1.0 + half_ele)
    e_factor = TIME_STEP / relative / (1.0 + half_ele)
    return e_retain, e_factor, h_retain, h_factor


def reference(bloch_index, material, permittivity, absorption_peak, source_sheet, waveform, electric_in, magnetic_in):
    depth = material.shape[2]
    rows = material.shape[0]
    e_retain, e_factor, h_retain, h_factor = coefficients(material, permittivity, absorption_peak, depth)
    plane = (jnp.arange(depth) == PML + 2).astype(jnp.float32)
    monitor = PML + 6
    angles = 2.0 * jnp.pi * bloch_index.astype(jnp.float32) / MPHASE

    def one_point(inputs):
        angle_pair, sheet_pair, electric_begin, magnetic_begin = inputs
        cos_x = jnp.cos(angle_pair[0])
        sin_x = jnp.sin(angle_pair[0])
        cos_y = jnp.cos(angle_pair[1])
        sin_y = jnp.sin(angle_pair[1])
        sheet = (sheet_pair[0][:, :, None] * plane, sheet_pair[1][:, :, None] * plane)

        def advance(fields, drive):
            electric, magnetic = fields
            beyond_y = rotate(slice_along(electric[1], 0, 1, 0), cos_x, sin_x)
            beyond_z = rotate(slice_along(electric[2], 0, 1, 0), cos_x, sin_x)
            change = electric_curl(electric, beyond_y, beyond_z, cos_y, sin_y)
            magnetic = tuple(relax(couple, change_part, h_retain, h_factor) for couple, change_part in zip(magnetic, change))
            behind_y = rotate(slice_along(magnetic[1], rows - 1, rows, 0), cos_x, -sin_x)
            behind_z = rotate(slice_along(magnetic[2], rows - 1, rows, 0), cos_x, -sin_x)
            change = magnetic_curl(magnetic, behind_y, behind_z, cos_y, sin_y)
            first_change = (change[0][0] - drive * sheet[0], change[0][1] - drive * sheet[1])
            change = (first_change, change[1], change[2])
            electric = tuple(relax(couple, change_part, e_retain, e_factor) for couple, change_part in zip(electric, change))
            return (electric, magnetic)

        def snapshot(fields, index):
            fields = lax.fori_loop(0, INTERVAL, lambda inner, held: advance(held, waveform[index * INTERVAL + inner]), fields)
            electric = fields[0]
            power = (electric[0][0][:, :, monitor] ** 2 + electric[0][1][:, :, monitor] ** 2
                     + electric[1][0][:, :, monitor] ** 2 + electric[1][1][:, :, monitor] ** 2)
            return fields, jnp.sum(power) / power.size

        electric_wide = electric_begin.astype(jnp.float32)
        magnetic_wide = magnetic_begin.astype(jnp.float32)
        start_e = tuple((electric_wide[2 * member], electric_wide[2 * member + 1]) for member in range(3))
        start_h = tuple((magnetic_wide[2 * member], magnetic_wide[2 * member + 1]) for member in range(3))
        final, powers = lax.scan(snapshot, (start_e, start_h), jnp.arange(NSNAP))
        electric, magnetic = final
        electric_stack = jnp.stack([values for couple in electric for values in couple], 0)
        magnetic_stack = jnp.stack([values for couple in magnetic for values in couple], 0)
        return electric_stack, magnetic_stack, powers

    electric_out, magnetic_out, reflected = lax.map(one_point, (angles, source_sheet, electric_in, magnetic_in))
    reflected_mean = jnp.sum(reflected, 0) / reflected.shape[0]
    return electric_out, magnetic_out, reflected, reflected_mean
```

```python
import jax
import jax.numpy as jnp
from jax import lax
from jax.experimental import pallas as pl
from jax.experimental.pallas import tpu as pltpu
from jax.sharding import PartitionSpec as P

PML = 16
INTERVAL = 5
MPHASE = 64
NMAT = 3
TIME_STEP = 0.5
MESH = pl.DeviceIdType.MESH


def rotate(couple, cosine, sine):
    return (couple[0] * cosine - couple[1] * sine, couple[0] * sine + couple[1] * cosine)


def minus(left, right):
    return (left[0] - right[0], left[1] - right[1])


def plus(left, right):
    return (left[0] + right[0], left[1] + right[1])


def relax(couple, change, keep, gain):
    return tuple(keep * c + gain * d for c, d in zip(couple, change))


def kernel(
    bloch_in,
    perm_in,
    peak_in,
    wave_in,
    material_in,
    sheet_in,
    e_hbm,
    h_hbm,
    e_ref,
    h_ref,
    power_ref,
    bloch_ref,
    perm_ref,
    peak_ref,
    wave_ref,
    material_ref,
    sheet_ref,
    e_in,
    h_in,
    report_ref,
    got_report,
    keep_ref,
    gain_ref,
    drive_ref,
    out_e,
    out_w,
    got_e,
    got_w,
    tiny_e,
    tiny_w,
    got_tiny_e,
    got_tiny_w,
    send_e,
    send_w,
    recv_e,
    recv_w,
    send_tiny,
    recv_tiny,
    load_sem,
    send_report,
    recv_report,
    entered,
):
    rows, width, depth = material_ref.shape
    steps = wave_ref.shape[0]
    slabs = lax.axis_size("sp")
    slab = lax.axis_index("sp")
    upper = lax.rem(slab + 1, slabs)
    lower = lax.rem(slab + slabs - 1, slabs)

    groups = lax.axis_size("ka")
    group = lax.axis_index("ka")
    everyone = groups * slabs
    me = group * slabs + slab

    def place(at):
        return {"ka": lax.div(at, slabs), "sp": lax.rem(at, slabs)}

    last_row = rows - 1
    loads = [
        pltpu.make_async_copy(src, dst, load_sem.at[at])
        for at, (src, dst) in enumerate(
            (
                (e_hbm.at[0, :, 0], e_in.at[0, :, 0]),
                (e_hbm.at[0, :, last_row], e_in.at[0, :, last_row]),
                (h_hbm.at[0, :, last_row], h_in.at[0, :, last_row]),
                (h_hbm.at[0, :, 0], h_in.at[0, :, 0]),
                (bloch_in, bloch_ref),
                (perm_in, perm_ref),
                (peak_in, peak_ref),
                (wave_in, wave_ref),
                (e_hbm.at[0, :, 1:last_row], e_in.at[0, :, 1:last_row]),
                (h_hbm.at[0, :, 1:last_row], h_in.at[0, :, 1:last_row]),
                (material_in, material_ref),
                (sheet_in, sheet_ref),
            )
        )
    ]
    for load in loads:
        load.start()

    barrier = pltpu.get_barrier_semaphore()

    def greet(other):
        pl.semaphore_signal(barrier, inc=1, device_id=place(other), device_id_type=MESH)

    bits = everyone.bit_length() - 1
    hypercube = everyone == 1 << bits
    rounds = bits - 1 if hypercube else 0
    greeted = bits + 2 if hypercube else everyone - 1

    def partner(bit):
        return me + (1 << bit) * (1 - 2 * lax.rem(lax.div(me, 1 << bit), 2))

    if hypercube:
        greet(group * slabs + lower)
        greet(group * slabs + upper)
        for bit in range(bits):
            greet(partner(bit))
    else:

        def greet_at(offset, carry):
            greet(lax.rem(me + offset, everyone))
            return carry

        lax.fori_loop(1, everyone, greet_at, 0)

    def spread(turn):
        pl.semaphore_signal(
            entered.at[turn], inc=1, device_id=place(partner(turn)), device_id_type=MESH
        )

    def learn(turn):
        pl.semaphore_wait(entered.at[turn], 1)

    for load in loads[4:8]:
        load.wait()

    height = lax.broadcasted_iota(jnp.int32, (8, depth), 1).astype(jnp.float32)
    low_depth = jnp.maximum(PML - height, 0.0) / PML
    high_depth = jnp.maximum(height - (depth - 1 - PML), 0.0) / PML
    conduct = peak_ref[0] * (
        low_depth * low_depth * low_depth + high_depth * high_depth * high_depth
    )
    half_mag = conduct * (0.5 * TIME_STEP)
    h_keep = ((1.0 - half_mag) / (1.0 + half_mag))[0:1]
    h_gain = (-TIME_STEP / (1.0 + half_mag))[0:1]
    tables = []
    for level in range(NMAT):
        relative = jnp.full((8, depth), perm_ref[level], jnp.float32)
        half_ele = conduct * (0.5 * TIME_STEP) / relative
        tables.append(
            (
                ((1.0 - half_ele) / (1.0 + half_ele))[0:1],
                (TIME_STEP / relative / (1.0 + half_ele))[0:1],
            )
        )

    def trig(member):
        angle = jnp.full((8, depth), bloch_ref[0, member], jnp.int32).astype(jnp.float32)
        angle = 2.0 * jnp.pi * angle / MPHASE
        return jnp.cos(angle)[0:1], jnp.sin(angle)[0:1]

    cos_x, sin_x = trig(0)
    cos_y, sin_y = trig(1)
    at_end = (slab == slabs - 1).astype(jnp.float32)
    at_start = (slab == 0).astype(jnp.float32)
    end_cos = at_end * cos_x + (1.0 - at_end)
    end_sin = at_end * sin_x
    start_cos = at_start * cos_x + (1.0 - at_start)
    start_sin = -at_start * sin_x

    lane = lax.broadcasted_iota(jnp.int32, (width, depth), 1)
    last_lane = lane == depth - 1
    first_lane = lane == 0
    sub = lax.broadcasted_iota(jnp.int32, (8, depth), 0)

    def above_z(couple):
        return tuple(jnp.where(last_lane, 0.0, pltpu.roll(v, depth - 1, 1)) for v in couple)

    def below_z(couple):
        return tuple(jnp.where(first_lane, 0.0, pltpu.roll(v, 1, 1)) for v in couple)

    def above_y(couple):
        moved = tuple(pltpu.roll(v, width - 1, 0) for v in couple)
        tail = tuple(v[width - 8 :] for v in moved)
        turned = rotate(tail, cos_y, sin_y)
        return tuple(
            jnp.concatenate([v[: width - 8], jnp.where(sub == 7, r, w)], axis=0)
            for v, r, w in zip(moved, turned, tail)
        )

    def below_y(couple):
        moved = tuple(pltpu.roll(v, 1, 0) for v in couple)
        head = tuple(v[:8] for v in moved)
        turned = rotate(head, cos_y, -sin_y)
        return tuple(
            jnp.concatenate([jnp.where(sub == 0, r, w), v[8:]], axis=0)
            for v, r, w in zip(moved, turned, head)
        )

    def get(ref, member, x):
        return (ref[0, 2 * member, x], ref[0, 2 * member + 1, x])

    def put(ref, member, x, couple):
        ref[0, 2 * member, x] = couple[0]
        ref[0, 2 * member + 1, x] = couple[1]

    def get_plane(ref, slot, member):
        return (ref[slot, 2 * member], ref[slot, 2 * member + 1])

    def put_plane(ref, slot, member, couple):
        ref[slot, 2 * member] = couple[0]
        ref[slot, 2 * member + 1] = couple[1]

    def hx_plane(x):
        ey, ez = get(e_ref, 1, x), get(e_ref, 2, x)
        change = minus(minus(above_y(ez), ez), minus(above_z(ey), ey))
        put(h_ref, 0, x, relax(get(h_ref, 0, x), change, h_keep, h_gain))

    def h_plane(x, carry):
        hx_plane(x)
        ex, ey, ez = get(e_ref, 0, x), get(e_ref, 1, x), get(e_ref, 2, x)
        dx_ez = minus(get(e_ref, 2, x + 1), ez)
        dx_ey = minus(get(e_ref, 1, x + 1), ey)
        change = minus(minus(above_z(ex), ex), dx_ez)
        put(h_ref, 1, x, relax(get(h_ref, 1, x), change, h_keep, h_gain))
        change = minus(dx_ey, minus(above_y(ex), ex))
        put(h_ref, 2, x, relax(get(h_ref, 2, x), change, h_keep, h_gain))
        return carry

    def partial_h(slot):
        x = rows - 1
        ex, ey, ez = get(e_ref, 0, x), get(e_ref, 1, x), get(e_ref, 2, x)
        change = plus(minus(above_z(ex), ex), ez)
        put_plane(out_w, slot, 0, relax(get(h_ref, 1, x), change, h_keep, h_gain))
        change = minus(minus(ex, above_y(ex)), ey)
        put_plane(out_w, slot, 1, relax(get(h_ref, 2, x), change, h_keep, h_gain))

    def complete_h(slot):
        x = rows - 1
        beyond_y = rotate(get_plane(got_e, slot, 0), end_cos, end_sin)
        beyond_z = rotate(get_plane(got_e, slot, 1), end_cos, end_sin)
        w_y, w_z = get_plane(out_w, slot, 0), get_plane(out_w, slot, 1)
        put(h_ref, 1, x, tuple(w - h_gain * b for w, b in zip(w_y, beyond_z)))
        put(h_ref, 2, x, tuple(w + h_gain * b for w, b in zip(w_z, beyond_y)))

    def new_ex(x, drive, hy, hz):
        change = minus(minus(hz, below_y(hz)), minus(hy, below_z(hy)))
        change = (change[0] - drive * drive_ref[0, x], change[1] - drive * drive_ref[1, x])
        return relax(get(e_ref, 0, x), change, keep_ref[x], gain_ref[x])

    def new_ey(x, hx, hz, hz_prev):
        change = minus(minus(hx, below_z(hx)), minus(hz, hz_prev))
        return relax(get(e_ref, 1, x), change, keep_ref[x], gain_ref[x])

    def new_ez(x, hx, hy, hy_prev):
        change = minus(minus(hy, hy_prev), minus(hx, below_y(hx)))
        return relax(get(e_ref, 2, x), change, keep_ref[x], gain_ref[x])

    def e_update(x, drive, hy_prev, hz_prev):
        hx, hy, hz = get(h_ref, 0, x), get(h_ref, 1, x), get(h_ref, 2, x)
        put(e_ref, 0, x, new_ex(x, drive, hy, hz))
        ey = new_ey(x, hx, hz, hz_prev)
        put(e_ref, 1, x, ey)
        ez = new_ez(x, hx, hy, hy_prev)
        put(e_ref, 2, x, ez)
        return ey, ez

    def e_first(slot, drive):
        ey, ez = get(e_ref, 1, 0), get(e_ref, 2, 0)
        turned_y = rotate(get_plane(got_w, slot, 0), start_cos, start_sin)
        turned_z = rotate(get_plane(got_w, slot, 1), start_cos, start_sin)
        hy_prev = tuple(w - h_gain * e for w, e in zip(turned_y, ez))
        hz_prev = tuple(w + h_gain * e for w, e in zip(turned_z, ey))
        return e_update(0, drive, hy_prev, hz_prev)

    def copy_e(slot):
        return pltpu.make_async_remote_copy(
            src_ref=out_e.at[slot],
            dst_ref=got_e.at[slot],
            send_sem=send_e.at[slot],
            recv_sem=recv_e.at[slot],
            device_id={"sp": lower},
            device_id_type=MESH,
        )

    def copy_w(slot):
        return pltpu.make_async_remote_copy(
            src_ref=out_w.at[slot],
            dst_ref=got_w.at[slot],
            send_sem=send_w.at[slot],
            recv_sem=recv_w.at[slot],
            device_id={"sp": upper},
            device_id_type=MESH,
        )

    square = lax.broadcasted_iota(jnp.int32, (width, width), 0) == lax.broadcasted_iota(
        jnp.int32, (width, width), 1
    )
    monitor = PML + 6

    def row_of(value, z):
        column = jnp.sum(jnp.where(lane == z, value, 0.0), axis=1, keepdims=True)
        return jnp.sum(jnp.where(square, column, 0.0), axis=0, keepdims=True)

    def at_lane(row, z):
        column = jnp.sum(jnp.where(square, row, 0.0), axis=1, keepdims=True)
        return jnp.where(lane == z, column, 0.0)

    def copy_tiny(src, dst, at, other):
        return pltpu.make_async_remote_copy(
            src_ref=src,
            dst_ref=dst,
            send_sem=send_tiny.at[at],
            recv_sem=recv_tiny.at[at],
            device_id={"sp": other},
            device_id_type=MESH,
        )

    def copy_tiny_e():
        return copy_tiny(tiny_e, got_tiny_e, 0, lower)

    def copy_tiny_w():
        return copy_tiny(tiny_w, got_tiny_w, 1, upper)

    def widen(x, carry):
        for member in range(6):
            e_ref[0, member, x] = e_in[0, member, x].astype(jnp.float32)
            h_ref[0, member, x] = h_in[0, member, x].astype(jnp.float32)
        return carry

    loads[0].wait()
    for member in range(4):
        out_e[0, member] = e_in[0, 2 + member, 0].astype(jnp.float32)
    pl.semaphore_wait(barrier, greeted)
    copy_e(0).start()
    for load in loads[1:4]:
        load.wait()
    widen(rows - 1, 0)
    partial_h(0)
    copy_w(0).start()
    widen(0, 0)
    for load in loads[8:]:
        load.wait()
    lax.fori_loop(1, rows - 1, widen, 0)

    report_ref[...] = jnp.zeros_like(report_ref)

    def prepare(x, carry):
        kind = material_ref[x]
        keep, gain = tables[0]
        for level in range(1, NMAT):
            keep = jnp.where(kind == level, tables[level][0], keep)
            gain = jnp.where(kind == level, tables[level][1], gain)
        keep_ref[x] = keep
        gain_ref[x] = gain
        for part in range(2):
            row = sheet_ref[0, part, pl.ds(x, 1), :]
            column = jnp.sum(jnp.where(square, row, 0.0), axis=1, keepdims=True)
            drive_ref[part, x] = jnp.where(lane == PML + 2, column, 0.0)
        return carry

    lax.fori_loop(0, rows, prepare, 0)

    def power(x, total):
        for member in range(4):
            value = e_ref[0, member, x]
            total = total + value * value
        return total

    row_lane = lax.broadcasted_iota(jnp.int32, (1, depth), 1)
    empty = jnp.zeros((width, depth), jnp.float32)
    last_snapshot = steps % INTERVAL == 0

    def note(total, at):
        amount = jnp.sum(jnp.where(lane == monitor, total, 0.0), axis=0, keepdims=True)
        amount = jnp.sum(amount, axis=1, keepdims=True)
        report_ref[...] += jnp.where(row_lane == at, amount, 0.0)

    def step(t, carry):
        slot = lax.rem(t, 2)
        later = lax.rem(t + 1, 2)
        drive = wave_ref[t]
        even = slot == 0
        snapshot = lax.rem(t + 1, INTERVAL) == 0
        before_last = t == steps - 2

        def left():
            copy_w(slot).wait_recv()
            ey, ez = e_first(slot, drive)

            @pl.when(t >= 1)
            def _():
                copy_e(later).wait_send()

            put_plane(out_e, later, 0, ey)
            put_plane(out_e, later, 1, ez)

            if last_snapshot:

                @pl.when(before_last)
                def _():
                    for part in range(2):
                        tiny_e[part : part + 1] = row_of(ey[part], monitor)
                        tiny_e[2 + part : 3 + part] = row_of(ez[part], monitor)
                        tiny_e[4 + part : 5 + part] = row_of(ez[part], monitor - 1)
                    copy_tiny_e().start()

            copy_e(later).start()

        def right():
            copy_e(slot).wait_recv()
            complete_h(slot)
            e_update(rows - 1, drive, get(h_ref, 1, rows - 2), get(h_ref, 2, rows - 2))

            @pl.when(t >= 1)
            def _():
                copy_w(later).wait_send()

            partial_h(later)

            if last_snapshot:

                @pl.when(before_last)
                def _():
                    for part in range(2):
                        tiny_w[part : part + 1] = row_of(out_w[later, 2 + part], monitor)
                    copy_tiny_w().start()

            copy_w(later).start()

        def inner(x, held):
            e_update(x, drive, get(h_ref, 1, x - 1), get(h_ref, 2, x - 1))
            return held

        for turn in range(min(rounds, steps - 1)):

            @pl.when(t == turn)
            def _():
                if turn > 0:
                    learn(turn - 1)
                spread(turn)

        lax.fori_loop(0, rows - 1, h_plane, 0)
        hx_plane(rows - 1)
        pl.when(even)(right)
        pl.when(jnp.logical_not(even))(left)
        lax.fori_loop(1, rows - 1, inner, 0)
        pl.when(even)(left)
        pl.when(jnp.logical_not(even))(right)

        @pl.when(snapshot)
        def _():
            note(lax.fori_loop(0, rows, power, empty), lax.div(t, INTERVAL))

        return carry

    lax.fori_loop(0, steps - 1, step, 0)
    for turn in range(min(rounds, steps - 1), rounds):
        if turn > 0:
            learn(turn - 1)
        spread(turn)
    if rounds > 0:
        learn(rounds - 1)

    def tell(offset):
        return pltpu.make_async_remote_copy(
            src_ref=report_ref,
            dst_ref=got_report.at[me],
            send_sem=send_report,
            recv_sem=recv_report,
            device_id=place(lax.rem(me + offset, everyone)),
            device_id_type=MESH,
        )

    def tell_start(offset, carry):
        tell(offset).start()
        return carry

    slot = (steps - 1) % 2
    drive = wave_ref[steps - 1]

    def inner_power(x, total):
        e_update(x, drive, get(h_ref, 1, x - 1), get(h_ref, 2, x - 1))
        return power(x, total)

    lax.fori_loop(0, rows - 1, h_plane, 0)
    hx_plane(rows - 1)
    total = lax.fori_loop(1, rows - 1, inner_power, empty)
    if last_snapshot:

        def unpack(ref, at, z):
            return tuple(at_lane(ref[at + part : at + part + 1], z) for part in range(2))

        copy_tiny_w().wait_recv()
        turned = rotate(unpack(got_tiny_w, 0, monitor), start_cos, start_sin)
        hz_prev = tuple(w + h_gain * e for w, e in zip(turned, get(e_ref, 1, 0)))
        hx, hy, hz = get(h_ref, 0, 0), get(h_ref, 1, 0), get(h_ref, 2, 0)
        for value in new_ex(0, drive, hy, hz) + new_ey(0, hx, hz, hz_prev):
            total = total + value * value

        copy_tiny_e().wait_recv()
        x = rows - 1
        beyond_y = rotate(unpack(got_tiny_e, 0, monitor), end_cos, end_sin)
        beyond_z = plus(unpack(got_tiny_e, 2, monitor), unpack(got_tiny_e, 4, monitor - 1))
        beyond_z = rotate(beyond_z, end_cos, end_sin)
        w_y, w_z = get_plane(out_w, slot, 0), get_plane(out_w, slot, 1)
        hy = tuple(w - h_gain * b for w, b in zip(w_y, beyond_z))
        hz = tuple(w + h_gain * b for w, b in zip(w_z, beyond_y))
        hx = get(h_ref, 0, x)
        for value in new_ex(x, drive, hy, hz) + new_ey(x, hx, hz, get(h_ref, 2, x - 1)):
            total = total + value * value
        note(total, steps // INTERVAL - 1)

    lax.fori_loop(1, everyone, tell_start, 0)
    got_report[me] = report_ref[...]

    def last_left():
        copy_w(slot).wait_recv()
        e_first(slot, drive)

    def last_right():
        copy_e(slot).wait_recv()
        complete_h(slot)
        e_update(rows - 1, drive, get(h_ref, 1, rows - 2), get(h_ref, 2, rows - 2))

    for side in (last_left, last_right) if slot else (last_right, last_left):
        side()
    for t in range(max(steps - 2, 0), steps):
        copy_e(t % 2).wait_send()
        copy_w(t % 2).wait_send()
    if last_snapshot:
        copy_tiny_e().wait_send()
        copy_tiny_w().wait_send()
    everything = got_report.at[pl.ds(0, everyone - 1)]
    pltpu.make_async_copy(everything, everything, recv_report).wait()
    pltpu.make_async_copy(everything, everything, send_report).wait()

    def gather(at, held):
        return held + got_report[group * slabs + at]

    ours = lax.fori_loop(0, slabs, gather, jnp.zeros((1, depth), jnp.float32))
    total = jnp.sum(got_report[...], axis=0)
    cells = rows * slabs * width
    power_ref[0:1] = ours / cells
    power_ref[1:2] = total / cells / groups


def write_out(e_ref, h_ref, power_ref, e_out, h_out, reflected_out, mean_out, own, mean, sems):
    members = e_ref.shape[1]
    snaps = mean.shape[0]
    writes = [
        pltpu.make_async_copy(src.at[0, member], dst.at[0, member], sems.at[at, member])
        for at, (src, dst) in enumerate(((e_ref, e_out), (h_ref, h_out)))
        for member in range(members)
    ]
    for write in writes:
        write.start()
    lane = lax.broadcasted_iota(jnp.int32, (1, power_ref.shape[1]), 1)
    for at in range(snaps):
        own[0, at] = jnp.sum(jnp.where(lane == at, power_ref[0:1], 0.0))
        mean[at] = jnp.sum(jnp.where(lane == at, power_ref[1:2], 0.0))
    small = [
        pltpu.make_async_copy(own, reflected_out, sems.at[0, members]),
        pltpu.make_async_copy(mean, mean_out, sems.at[1, members]),
    ]
    for write in small:
        write.start()
    for write in writes + small:
        write.wait()


def one_point(bloch, material, permittivity, peak, sheet, waveform, electric, magnetic):
    rows, width, depth = material.shape
    snaps = waveform.shape[0] // INTERVAL
    everyone = lax.axis_size("ka") * lax.axis_size("sp")
    hbm = pl.BlockSpec(memory_space=pltpu.HBM)
    vmem = pl.BlockSpec(memory_space=pltpu.VMEM)
    plane = (2, 4, width, depth)
    f32 = jnp.float32
    tiny = [pltpu.VMEM((rows_of_tiny, width), f32) for rows_of_tiny in (6, 2, 6, 2)]
    electric_end, magnetic_end, power = pl.pallas_call(
        kernel,
        out_shape=(
            jax.ShapeDtypeStruct(electric.shape, f32),
            jax.ShapeDtypeStruct(magnetic.shape, f32),
            jax.ShapeDtypeStruct((8, depth), f32),
        ),
        in_specs=[hbm] * 8,
        out_specs=(vmem, vmem, vmem),
        scratch_shapes=[
            pltpu.SMEM(bloch.shape, jnp.int32),
            pltpu.SMEM(permittivity.shape, f32),
            pltpu.SMEM(peak.shape, f32),
            pltpu.SMEM(waveform.shape, f32),
            pltpu.VMEM(material.shape, jnp.int32),
            pltpu.VMEM(sheet.shape, f32),
            pltpu.VMEM(electric.shape, electric.dtype),
            pltpu.VMEM(magnetic.shape, magnetic.dtype),
            pltpu.VMEM((1, depth), f32),
            pltpu.VMEM((everyone, 1, depth), f32),
            pltpu.VMEM((rows, width, depth), f32),
            pltpu.VMEM((rows, width, depth), f32),
            pltpu.VMEM((2, rows, width, depth), f32),
            pltpu.VMEM(plane, f32),
            pltpu.VMEM(plane, f32),
            pltpu.VMEM(plane, f32),
            pltpu.VMEM(plane, f32),
            *tiny,
            pltpu.SemaphoreType.DMA((2,)),
            pltpu.SemaphoreType.DMA((2,)),
            pltpu.SemaphoreType.DMA((2,)),
            pltpu.SemaphoreType.DMA((2,)),
            pltpu.SemaphoreType.DMA((2,)),
            pltpu.SemaphoreType.DMA((2,)),
            pltpu.SemaphoreType.DMA((12,)),
            pltpu.SemaphoreType.DMA,
            pltpu.SemaphoreType.DMA,
            pltpu.SemaphoreType.REGULAR((max(everyone.bit_length(), 1),)),
        ],
        compiler_params=pltpu.CompilerParams(
            collective_id=0, has_side_effects=True, vmem_limit_bytes=40 * 1024 * 1024
        ),
    )(*((v if v.shape == (1,) else pltpu.with_memory_space_constraint(v, pltpu.HBM)) for v in (bloch, permittivity, peak, waveform, material, sheet, electric, magnetic)))
    return pl.pallas_call(
        write_out,
        out_shape=(
            pltpu.HBM(electric.shape, f32),
            pltpu.HBM(magnetic.shape, f32),
            pltpu.HBM((1, snaps), f32),
            pltpu.HBM((snaps,), f32),
        ),
        in_specs=[vmem] * 3,
        out_specs=(hbm,) * 4,
        scratch_shapes=[
            pltpu.SMEM((1, snaps), f32),
            pltpu.SMEM((snaps,), f32),
            pltpu.SemaphoreType.DMA((2, electric.shape[1] + 1)),
        ],
        compiler_params=pltpu.CompilerParams(vmem_limit_bytes=1024 * 1024),
    )(electric_end, magnetic_end, power)


def on_device(
    bloch_index,
    material,
    permittivity,
    absorption_peak,
    source_sheet,
    waveform,
    electric_in,
    magnetic_in,
):
    points = bloch_index.shape[0]
    results = [
        one_point(
            bloch_index[p : p + 1],
            material,
            permittivity,
            absorption_peak,
            source_sheet[p : p + 1],
            waveform,
            electric_in[p : p + 1],
            magnetic_in[p : p + 1],
        )
        for p in range(points)
    ]
    if points == 1:
        return results[0]
    electric_out, magnetic_out, reflected, mean = (list(r) for r in zip(*results))
    return (
        jnp.concatenate(electric_out, 0),
        jnp.concatenate(magnetic_out, 0),
        jnp.concatenate(reflected, 0),
        sum(mean) / points,
    )


def solution(mesh):
    in_specs = (
        P("ka", None),
        P("sp", None, None),
        P(),
        P(),
        P("ka", None, "sp", None),
        P(),
        P("ka", None, "sp", None, None),
        P("ka", None, "sp", None, None),
    )
    out_specs = (
        P("ka", None, "sp", None, None),
        P("ka", None, "sp", None, None),
        P("ka", None),
        P(),
    )
    return jax.shard_map(
        on_device, mesh=mesh, in_specs=in_specs, out_specs=out_specs, check_vma=False
    )
```

```python
import jax
import jax.numpy as jnp
from jax import lax
from jax.experimental import pallas as pl
from jax.experimental.pallas import tpu as pltpu
from jax.sharding import PartitionSpec as P

PML = 16
INTERVAL = 5
MPHASE = 64
NMAT = 3
TIME_STEP = 0.5
MESH = pl.DeviceIdType.MESH


def rotate(couple, cosine, sine):
    return (couple[0] * cosine - couple[1] * sine, couple[0] * sine + couple[1] * cosine)


def minus(left, right):
    return (left[0] - right[0], left[1] - right[1])


def plus(left, right):
    return (left[0] + right[0], left[1] + right[1])


def relax(couple, change, keep, gain):
    return tuple(keep * c + gain * d for c, d in zip(couple, change))


def kernel(
    bloch_in,
    perm_in,
    peak_in,
    wave_in,
    material_in,
    sheet_in,
    e_hbm,
    h_hbm,
    e_ref,
    h_ref,
    power_ref,
    bloch_ref,
    perm_ref,
    peak_ref,
    wave_ref,
    material_ref,
    sheet_ref,
    e_in,
    h_in,
    report_ref,
    got_report,
    keep_ref,
    gain_ref,
    drive_ref,
    out_e,
    out_w,
    got_e,
    got_w,
    tiny,
    got_tiny,
    ahead_ref,
    send_e,
    send_w,
    recv_e,
    recv_w,
    send_tiny,
    recv_tiny,
    load_sem,
    send_report,
    recv_report,
    entered,
):
    rows, width, depth = material_ref.shape
    steps = wave_ref.shape[0]
    slabs = lax.axis_size("sp")
    slab = lax.axis_index("sp")
    upper = lax.rem(slab + 1, slabs)
    lower = lax.rem(slab + slabs - 1, slabs)

    groups = lax.axis_size("ka")
    group = lax.axis_index("ka")
    everyone = groups * slabs
    me = group * slabs + slab

    def place(at):
        return {"ka": lax.div(at, slabs), "sp": lax.rem(at, slabs)}

    last_row = rows - 1
    loads = [
        pltpu.make_async_copy(src, dst, load_sem.at[at])
        for at, (src, dst) in enumerate(
            (
                (e_hbm.at[0, :, 0], e_in.at[0, :, 0]),
                (e_hbm.at[0, :, last_row], e_in.at[0, :, last_row]),
                (h_hbm.at[0, :, last_row], h_in.at[0, :, last_row]),
                (h_hbm.at[0, :, 0], h_in.at[0, :, 0]),
                (bloch_in, bloch_ref),
                (perm_in, perm_ref),
                (peak_in, peak_ref),
                (wave_in, wave_ref),
                (e_hbm.at[0, :, 1:last_row], e_in.at[0, :, 1:last_row]),
                (h_hbm.at[0, :, 1:last_row], h_in.at[0, :, 1:last_row]),
                (material_in, material_ref),
                (sheet_in, sheet_ref),
            )
        )
    ]
    for load in loads:
        load.start()

    barrier = pltpu.get_barrier_semaphore()

    def greet(other):
        pl.semaphore_signal(barrier, inc=1, device_id=place(other), device_id_type=MESH)

    bits = everyone.bit_length() - 1
    hypercube = everyone == 1 << bits
    rounds = bits - 1 if hypercube else 0
    greeted = bits + 2 if hypercube else everyone - 1

    def partner(bit):
        return me + (1 << bit) * (1 - 2 * lax.rem(lax.div(me, 1 << bit), 2))

    if hypercube:
        greet(group * slabs + lower)
        greet(group * slabs + upper)
        for bit in range(bits):
            greet(partner(bit))
    else:

        def greet_at(offset, carry):
            greet(lax.rem(me + offset, everyone))
            return carry

        lax.fori_loop(1, everyone, greet_at, 0)

    def spread(turn):
        pl.semaphore_signal(
            entered.at[turn], inc=1, device_id=place(partner(turn)), device_id_type=MESH
        )

    def learn(turn):
        pl.semaphore_wait(entered.at[turn], 1)

    for load in loads[4:8]:
        load.wait()

    height = lax.broadcasted_iota(jnp.int32, (8, depth), 1).astype(jnp.float32)
    low_depth = jnp.maximum(PML - height, 0.0) / PML
    high_depth = jnp.maximum(height - (depth - 1 - PML), 0.0) / PML
    conduct = peak_ref[0] * (
        low_depth * low_depth * low_depth + high_depth * high_depth * high_depth
    )
    half_mag = conduct * (0.5 * TIME_STEP)
    h_keep = ((1.0 - half_mag) / (1.0 + half_mag))[0:1]
    h_gain = (-TIME_STEP / (1.0 + half_mag))[0:1]
    tables = []
    for level in range(NMAT):
        relative = jnp.full((8, depth), perm_ref[level], jnp.float32)
        half_ele = conduct * (0.5 * TIME_STEP) / relative
        tables.append(
            (
                ((1.0 - half_ele) / (1.0 + half_ele))[0:1],
                (TIME_STEP / relative / (1.0 + half_ele))[0:1],
            )
        )

    def trig(member):
        angle = jnp.full((8, depth), bloch_ref[0, member], jnp.int32).astype(jnp.float32)
        angle = 2.0 * jnp.pi * angle / MPHASE
        return jnp.cos(angle)[0:1], jnp.sin(angle)[0:1]

    cos_x, sin_x = trig(0)
    cos_y, sin_y = trig(1)
    at_end = (slab == slabs - 1).astype(jnp.float32)
    at_start = (slab == 0).astype(jnp.float32)
    end_cos = at_end * cos_x + (1.0 - at_end)
    end_sin = at_end * sin_x
    start_cos = at_start * cos_x + (1.0 - at_start)
    start_sin = -at_start * sin_x

    lane = lax.broadcasted_iota(jnp.int32, (width, depth), 1)
    last_lane = lane == depth - 1
    first_lane = lane == 0
    sub = lax.broadcasted_iota(jnp.int32, (8, depth), 0)

    def above_z(couple):
        return tuple(jnp.where(last_lane, 0.0, pltpu.roll(v, depth - 1, 1)) for v in couple)

    def below_z(couple):
        return tuple(jnp.where(first_lane, 0.0, pltpu.roll(v, 1, 1)) for v in couple)

    def above_y(couple):
        moved = tuple(pltpu.roll(v, width - 1, 0) for v in couple)
        tail = tuple(v[width - 8 :] for v in moved)
        turned = rotate(tail, cos_y, sin_y)
        return tuple(
            jnp.concatenate([v[: width - 8], jnp.where(sub == 7, r, w)], axis=0)
            for v, r, w in zip(moved, turned, tail)
        )

    def below_y(couple):
        moved = tuple(pltpu.roll(v, 1, 0) for v in couple)
        head = tuple(v[:8] for v in moved)
        turned = rotate(head, cos_y, -sin_y)
        return tuple(
            jnp.concatenate([jnp.where(sub == 0, r, w), v[8:]], axis=0)
            for v, r, w in zip(moved, turned, head)
        )

    def get(ref, member, x):
        return (ref[0, 2 * member, x], ref[0, 2 * member + 1, x])

    def put(ref, member, x, couple):
        ref[0, 2 * member, x] = couple[0]
        ref[0, 2 * member + 1, x] = couple[1]

    def get_plane(ref, slot, member):
        return (ref[slot, 2 * member], ref[slot, 2 * member + 1])

    def put_plane(ref, slot, member, couple):
        ref[slot, 2 * member] = couple[0]
        ref[slot, 2 * member + 1] = couple[1]

    def new_hx(x, ey, ez):
        change = minus(minus(above_y(ez), ez), minus(above_z(ey), ey))
        return relax(get(h_ref, 0, x), change, h_keep, h_gain)

    def new_hy(x, ex, ez, ez_next):
        change = minus(minus(above_z(ex), ex), minus(ez_next, ez))
        return relax(get(h_ref, 1, x), change, h_keep, h_gain)

    def new_hz(x, ex, ey, ey_next):
        change = minus(minus(ey_next, ey), minus(above_y(ex), ex))
        return relax(get(h_ref, 2, x), change, h_keep, h_gain)

    def hx_plane(x):
        put(h_ref, 0, x, new_hx(x, get(e_ref, 1, x), get(e_ref, 2, x)))

    def h_plane(x):
        ex, ey, ez = get(e_ref, 0, x), get(e_ref, 1, x), get(e_ref, 2, x)
        put(h_ref, 0, x, new_hx(x, ey, ez))
        put(h_ref, 1, x, new_hy(x, ex, ez, get(e_ref, 2, x + 1)))
        put(h_ref, 2, x, new_hz(x, ex, ey, get(e_ref, 1, x + 1)))

    def partial_h(slot):
        x = rows - 1
        ex, ey, ez = get(e_ref, 0, x), get(e_ref, 1, x), get(e_ref, 2, x)
        change = plus(minus(above_z(ex), ex), ez)
        put_plane(out_w, slot, 0, relax(get(h_ref, 1, x), change, h_keep, h_gain))
        change = minus(minus(ex, above_y(ex)), ey)
        put_plane(out_w, slot, 1, relax(get(h_ref, 2, x), change, h_keep, h_gain))

    def complete_h(slot):
        x = rows - 1
        beyond_y = rotate(get_plane(got_e, slot, 0), end_cos, end_sin)
        beyond_z = rotate(get_plane(got_e, slot, 1), end_cos, end_sin)
        w_y, w_z = get_plane(out_w, slot, 0), get_plane(out_w, slot, 1)
        put(h_ref, 1, x, tuple(w - h_gain * b for w, b in zip(w_y, beyond_z)))
        put(h_ref, 2, x, tuple(w + h_gain * b for w, b in zip(w_z, beyond_y)))

    def new_ex(x, drive, hy, hz):
        change = minus(minus(hz, below_y(hz)), minus(hy, below_z(hy)))
        change = (change[0] - drive * drive_ref[0, x], change[1] - drive * drive_ref[1, x])
        return relax(get(e_ref, 0, x), change, keep_ref[x], gain_ref[x])

    def new_ey(x, ey, hx, hz, hz_prev):
        change = minus(minus(hx, below_z(hx)), minus(hz, hz_prev))
        return relax(ey, change, keep_ref[x], gain_ref[x])

    def new_ez(x, hx, hy, hy_prev):
        change = minus(minus(hy, hy_prev), minus(hx, below_y(hx)))
        return relax(get(e_ref, 2, x), change, keep_ref[x], gain_ref[x])

    def e_update(x, drive, hy_prev, hz_prev):
        hx, hy, hz = get(h_ref, 0, x), get(h_ref, 1, x), get(h_ref, 2, x)
        put(e_ref, 0, x, new_ex(x, drive, hy, hz))
        ey = new_ey(x, get(e_ref, 1, x), hx, hz, hz_prev)
        put(e_ref, 1, x, ey)
        ez = new_ez(x, hx, hy, hy_prev)
        put(e_ref, 2, x, ez)
        return ey, ez

    def beside(turned_y, turned_z, ey, ez):
        hy_prev = tuple(w - h_gain * e for w, e in zip(turned_y, ez))
        hz_prev = tuple(w + h_gain * e for w, e in zip(turned_z, ey))
        return hy_prev, hz_prev

    def got_beside(slot):
        turned_y = rotate(get_plane(got_w, slot, 0), start_cos, start_sin)
        turned_z = rotate(get_plane(got_w, slot, 1), start_cos, start_sin)
        return beside(turned_y, turned_z, get(e_ref, 1, 0), get(e_ref, 2, 0))

    def e_first(slot, drive):
        return e_update(0, drive, *got_beside(slot))

    def e_middle(x, drive):
        return e_update(x, drive, get(h_ref, 1, x - 1), get(h_ref, 2, x - 1))

    def copy_e(slot):
        return pltpu.make_async_remote_copy(
            src_ref=out_e.at[slot],
            dst_ref=got_e.at[slot],
            send_sem=send_e.at[slot],
            recv_sem=recv_e.at[slot],
            device_id={"sp": lower},
            device_id_type=MESH,
        )

    def copy_w(slot):
        return pltpu.make_async_remote_copy(
            src_ref=out_w.at[slot],
            dst_ref=got_w.at[slot],
            send_sem=send_w.at[slot],
            recv_sem=recv_w.at[slot],
            device_id={"sp": upper},
            device_id_type=MESH,
        )

    square = lax.broadcasted_iota(jnp.int32, (width, width), 0) == lax.broadcasted_iota(
        jnp.int32, (width, width), 1
    )
    monitor = PML + 6

    def row_of(value, z):
        column = jnp.sum(jnp.where(lane == z, value, 0.0), axis=1, keepdims=True)
        return jnp.sum(jnp.where(square, column, 0.0), axis=0, keepdims=True)

    def at_lane(row, z):
        column = jnp.sum(jnp.where(square, row, 0.0), axis=1, keepdims=True)
        return jnp.where(lane == z, column, 0.0)

    def copy_tiny(at, other):
        return pltpu.make_async_remote_copy(
            src_ref=tiny.at[at],
            dst_ref=got_tiny.at[at],
            send_sem=send_tiny.at[at],
            recv_sem=recv_tiny.at[at],
            device_id={"sp": other},
            device_id_type=MESH,
        )

    def pack(at, columns):
        for place_in, (couple, z) in enumerate(columns):
            for part in range(2):
                line = 2 * place_in + part
                tiny[at, line : line + 1] = row_of(couple[part], z)

    def unpack(at, place_in, z):
        lines = (2 * place_in, 2 * place_in + 1)
        return tuple(at_lane(got_tiny[at, line : line + 1], z) for line in lines)

    early_w, late_w, late_e = (copy_tiny(0, upper), copy_tiny(1, upper), copy_tiny(2, lower))

    def widen(x, carry):
        for member in range(6):
            e_ref[0, member, x] = e_in[0, member, x].astype(jnp.float32)
            h_ref[0, member, x] = h_in[0, member, x].astype(jnp.float32)
        return carry

    loads[0].wait()
    for member in range(4):
        out_e[0, member] = e_in[0, 2 + member, 0].astype(jnp.float32)
    pl.semaphore_wait(barrier, greeted)
    copy_e(0).start()
    for load in loads[1:4]:
        load.wait()
    widen(rows - 1, 0)
    partial_h(0)
    copy_w(0).start()
    widen(0, 0)
    for load in loads[8:]:
        load.wait()
    lax.fori_loop(1, rows - 1, widen, 0)

    report_ref[...] = jnp.zeros_like(report_ref)

    def prepare(x, carry):
        kind = material_ref[x]
        keep, gain = tables[0]
        for level in range(1, NMAT):
            keep = jnp.where(kind == level, tables[level][0], keep)
            gain = jnp.where(kind == level, tables[level][1], gain)
        keep_ref[x] = keep
        gain_ref[x] = gain
        for part in range(2):
            row = sheet_ref[0, part, pl.ds(x, 1), :]
            column = jnp.sum(jnp.where(square, row, 0.0), axis=1, keepdims=True)
            drive_ref[part, x] = jnp.where(lane == PML + 2, column, 0.0)
        return carry

    lax.fori_loop(0, rows, prepare, 0)

    def power(x, total):
        for member in range(4):
            value = e_ref[0, member, x]
            total = total + value * value
        return total

    row_lane = lax.broadcasted_iota(jnp.int32, (1, depth), 1)
    empty = jnp.zeros((width, depth), jnp.float32)
    assert steps % (2 * INTERVAL) == 0

    def note(total, at):
        amount = jnp.sum(jnp.where(lane == monitor, total, 0.0), axis=0, keepdims=True)
        amount = jnp.sum(amount, axis=1, keepdims=True)
        report_ref[...] += jnp.where(row_lane == at, amount, 0.0)

    def sides(t, slot, later, drive):
        def left():
            copy_w(slot).wait_recv()
            ey, ez = e_first(slot, drive)

            @pl.when(t >= 1)
            def _():
                copy_e(later).wait_send()

            put_plane(out_e, later, 0, ey)
            put_plane(out_e, later, 1, ez)
            copy_e(later).start()

        def right():
            copy_e(slot).wait_recv()
            complete_h(slot)
            e_middle(rows - 1, drive)

            @pl.when(t >= 1)
            def _():
                copy_w(later).wait_send()

            partial_h(later)

            @pl.when(t == steps - 3)
            def _():
                w_y, w_z = get_plane(out_w, later, 0), get_plane(out_w, later, 1)
                pack(
                    0,
                    [(w_z, monitor - 1), (w_z, monitor), (w_z, monitor + 1)]
                    + [(w_y, monitor - 1), (w_y, monitor)],
                )
                early_w.start()

            copy_w(later).start()

        return left, right

    def before_sides():
        h_plane(0)
        h_plane(1)
        h_plane(rows - 2)
        hx_plane(rows - 1)

    def between_sides(drive):
        def both(x, held):
            e_middle(x, drive)
            h_plane(x + 1)
            return held

        lax.fori_loop(1, rows - 3, both, 0)
        e_middle(rows - 3, drive)
        e_middle(rows - 2, drive)

    def step(t, carry):
        slot = lax.rem(t, 2)
        later = lax.rem(t + 1, 2)
        drive = wave_ref[t]
        even = slot == 0
        left, right = sides(t, slot, later, drive)

        for turn in range(min(rounds, steps - 2)):

            @pl.when(t == turn)
            def _():
                if turn > 0:
                    learn(turn - 1)
                spread(turn)

        before_sides()
        pl.when(even)(right)
        pl.when(jnp.logical_not(even))(left)
        between_sides(drive)
        pl.when(even)(left)
        pl.when(jnp.logical_not(even))(right)

        @pl.when(lax.rem(t + 1, INTERVAL) == 0)
        def _():
            note(lax.fori_loop(0, rows, power, empty), lax.div(t, INTERVAL))

        return carry

    lax.fori_loop(0, steps - 2, step, 0)
    for turn in range(min(rounds, steps - 2), rounds):
        if turn > 0:
            learn(turn - 1)
        spread(turn)
    if rounds > 0:
        learn(rounds - 1)

    def tell(offset):
        return pltpu.make_async_remote_copy(
            src_ref=report_ref,
            dst_ref=got_report.at[me],
            send_sem=send_report,
            recv_sem=recv_report,
            device_id=place(lax.rem(me + offset, everyone)),
            device_id_type=MESH,
        )

    def tell_start(offset, carry):
        tell(offset).start()
        return carry

    slot, later = (steps - 2) % 2, (steps - 1) % 2
    drive, last_drive = wave_ref[steps - 2], wave_ref[steps - 1]
    end = rows - 1
    before_sides()
    between_sides(drive)
    early_w.wait_recv()
    hx, hy, hz = get(h_ref, 0, 0), get(h_ref, 1, 0), get(h_ref, 2, 0)
    put(e_ref, 0, 0, new_ex(0, drive, hy, hz))
    w_z = plus(plus(unpack(0, 0, monitor - 1), unpack(0, 1, monitor)), unpack(0, 2, monitor + 1))
    w_y = plus(unpack(0, 3, monitor - 1), unpack(0, 4, monitor))
    ey, ez = get(e_ref, 1, 0), get(e_ref, 2, 0)
    hy_prev, hz_prev = beside(
        rotate(w_y, start_cos, start_sin), rotate(w_z, start_cos, start_sin), ey, ez
    )
    ey = new_ey(0, ey, hx, hz, hz_prev)
    ez = new_ez(0, hx, hy, hy_prev)
    put_plane(ahead_ref, 0, 0, ey)
    put_plane(ahead_ref, 0, 1, ez)
    pack(2, [(ey, monitor), (ez, monitor), (ez, monitor - 1)])
    late_e.start()

    copy_e(slot).wait_recv()
    complete_h(slot)
    e_middle(end, drive)
    copy_w(later).wait_send()
    partial_h(later)
    pack(1, [(get_plane(out_w, later, 1), monitor)])
    late_w.start()
    copy_w(later).start()

    h_plane(1)
    h_plane(2)

    def both(x, total):
        e_middle(x, last_drive)
        h_plane(x + 1)
        return power(x, total)

    total = lax.fori_loop(2, end - 1, both, empty)
    e_middle(end - 1, last_drive)
    total = power(end - 1, total)
    hx_plane(end)

    def first_plane():
        copy_w(slot).wait_recv()
        hx, hy, hz = get(h_ref, 0, 0), get(h_ref, 1, 0), get(h_ref, 2, 0)
        hy_prev, hz_prev = got_beside(slot)
        ey = new_ey(0, get(e_ref, 1, 0), hx, hz, hz_prev)
        ez = new_ez(0, hx, hy, hy_prev)
        put(e_ref, 1, 0, ey)
        put(e_ref, 2, 0, ez)
        copy_e(later).wait_send()
        put_plane(out_e, later, 0, ey)
        put_plane(out_e, later, 1, ez)
        copy_e(later).start()

    first_plane()
    ex, ey, ez = get(e_ref, 0, 0), get_plane(ahead_ref, 0, 0), get_plane(ahead_ref, 0, 1)
    hx = new_hx(0, ey, ez)
    hy = new_hy(0, ex, ez, get(e_ref, 2, 1))
    hz = new_hz(0, ex, ey, get(e_ref, 1, 1))
    hx1, hy1, hz1 = get(h_ref, 0, 1), get(h_ref, 1, 1), get(h_ref, 2, 1)
    late_w.wait_recv()
    hz_prev = rotate(unpack(1, 0, monitor), start_cos, start_sin)
    hz_prev = tuple(w + h_gain * e for w, e in zip(hz_prev, ey))
    for value in (
        new_ex(0, last_drive, hy, hz)
        + new_ey(0, ey, hx, hz, hz_prev)
        + new_ex(1, last_drive, hy1, hz1)
        + new_ey(1, get(e_ref, 1, 1), hx1, hz1, hz)
    ):
        total = total + value * value
    late_e.wait_recv()
    beyond_y = rotate(unpack(2, 0, monitor), end_cos, end_sin)
    beyond_z = plus(unpack(2, 1, monitor), unpack(2, 2, monitor - 1))
    beyond_z = rotate(beyond_z, end_cos, end_sin)
    w_y, w_z = get_plane(out_w, later, 0), get_plane(out_w, later, 1)
    hx = get(h_ref, 0, end)
    hy = tuple(w - h_gain * b for w, b in zip(w_y, beyond_z))
    hz = tuple(w + h_gain * b for w, b in zip(w_z, beyond_y))
    for value in new_ex(end, last_drive, hy, hz) + new_ey(
        end, get(e_ref, 1, end), hx, hz, get(h_ref, 2, end - 1)
    ):
        total = total + value * value
    note(total, steps // INTERVAL - 1)
    lax.fori_loop(1, everyone, tell_start, 0)
    got_report[me] = report_ref[...]

    h_plane(0)
    e_middle(1, last_drive)
    copy_w(later).wait_recv()
    e_first(later, last_drive)
    copy_e(later).wait_recv()
    complete_h(later)
    e_middle(end, last_drive)
    for at in range(2):
        copy_e(at).wait_send()
        copy_w(at).wait_send()
    for copy in (early_w, late_w, late_e):
        copy.wait_send()
    everything = got_report.at[pl.ds(0, everyone - 1)]
    pltpu.make_async_copy(everything, everything, recv_report).wait()
    pltpu.make_async_copy(everything, everything, send_report).wait()

    def gather(at, held):
        return held + got_report[group * slabs + at]

    ours = lax.fori_loop(0, slabs, gather, jnp.zeros((1, depth), jnp.float32))
    total = jnp.sum(got_report[...], axis=0)
    cells = rows * slabs * width
    power_ref[0:1] = ours / cells
    power_ref[1:2] = total / cells / groups


def write_out(e_ref, h_ref, power_ref, e_out, h_out, reflected_out, mean_out, own, mean, sems):
    members = e_ref.shape[1]
    snaps = mean.shape[0]
    writes = [
        pltpu.make_async_copy(src.at[0, member], dst.at[0, member], sems.at[at, member])
        for at, (src, dst) in enumerate(((e_ref, e_out), (h_ref, h_out)))
        for member in range(members)
    ]
    for write in writes:
        write.start()
    lane = lax.broadcasted_iota(jnp.int32, (1, power_ref.shape[1]), 1)
    for at in range(snaps):
        own[0, at] = jnp.sum(jnp.where(lane == at, power_ref[0:1], 0.0))
        mean[at] = jnp.sum(jnp.where(lane == at, power_ref[1:2], 0.0))
    small = [
        pltpu.make_async_copy(own, reflected_out, sems.at[0, members]),
        pltpu.make_async_copy(mean, mean_out, sems.at[1, members]),
    ]
    for write in small:
        write.start()
    for write in writes + small:
        write.wait()


def one_point(bloch, material, permittivity, peak, sheet, waveform, electric, magnetic):
    rows, width, depth = material.shape
    snaps = waveform.shape[0] // INTERVAL
    everyone = lax.axis_size("ka") * lax.axis_size("sp")
    hbm = pl.BlockSpec(memory_space=pltpu.HBM)
    vmem = pl.BlockSpec(memory_space=pltpu.VMEM)
    plane = (2, 4, width, depth)
    f32 = jnp.float32
    electric_end, magnetic_end, power = pl.pallas_call(
        kernel,
        out_shape=(
            jax.ShapeDtypeStruct(electric.shape, f32),
            jax.ShapeDtypeStruct(magnetic.shape, f32),
            jax.ShapeDtypeStruct((8, depth), f32),
        ),
        in_specs=[hbm] * 8,
        out_specs=(vmem, vmem, vmem),
        scratch_shapes=[
            pltpu.SMEM(bloch.shape, jnp.int32),
            pltpu.SMEM(permittivity.shape, f32),
            pltpu.SMEM(peak.shape, f32),
            pltpu.SMEM(waveform.shape, f32),
            pltpu.VMEM(material.shape, jnp.int32),
            pltpu.VMEM(sheet.shape, f32),
            pltpu.VMEM(electric.shape, electric.dtype),
            pltpu.VMEM(magnetic.shape, magnetic.dtype),
            pltpu.VMEM((1, depth), f32),
            pltpu.VMEM((everyone, 1, depth), f32),
            pltpu.VMEM((rows, width, depth), f32),
            pltpu.VMEM((rows, width, depth), f32),
            pltpu.VMEM((2, rows, width, depth), f32),
            pltpu.VMEM(plane, f32),
            pltpu.VMEM(plane, f32),
            pltpu.VMEM(plane, f32),
            pltpu.VMEM(plane, f32),
            pltpu.VMEM((3, 16, width), f32),
            pltpu.VMEM((3, 16, width), f32),
            pltpu.VMEM((1, 4, width, depth), f32),
            pltpu.SemaphoreType.DMA((2,)),
            pltpu.SemaphoreType.DMA((2,)),
            pltpu.SemaphoreType.DMA((2,)),
            pltpu.SemaphoreType.DMA((2,)),
            pltpu.SemaphoreType.DMA((3,)),
            pltpu.SemaphoreType.DMA((3,)),
            pltpu.SemaphoreType.DMA((12,)),
            pltpu.SemaphoreType.DMA,
            pltpu.SemaphoreType.DMA,
            pltpu.SemaphoreType.REGULAR((max(everyone.bit_length(), 1),)),
        ],
        compiler_params=pltpu.CompilerParams(
            collective_id=0, has_side_effects=True, vmem_limit_bytes=40 * 1024 * 1024
        ),
    )(*((v if v.shape == (1,) else pltpu.with_memory_space_constraint(v, pltpu.HBM)) for v in (bloch, permittivity, peak, waveform, material, sheet, electric, magnetic)))
    return pl.pallas_call(
        write_out,
        out_shape=(
            pltpu.HBM(electric.shape, f32),
            pltpu.HBM(magnetic.shape, f32),
            pltpu.HBM((1, snaps), f32),
            pltpu.HBM((snaps,), f32),
        ),
        in_specs=[vmem] * 3,
        out_specs=(hbm,) * 4,
        scratch_shapes=[
            pltpu.SMEM((1, snaps), f32),
            pltpu.SMEM((snaps,), f32),
            pltpu.SemaphoreType.DMA((2, electric.shape[1] + 1)),
        ],
        compiler_params=pltpu.CompilerParams(vmem_limit_bytes=1024 * 1024),
    )(electric_end, magnetic_end, power)


def on_device(
    bloch_index,
    material,
    permittivity,
    absorption_peak,
    source_sheet,
    waveform,
    electric_in,
    magnetic_in,
):
    points = bloch_index.shape[0]
    results = [
        one_point(
            bloch_index[p : p + 1],
            material,
            permittivity,
            absorption_peak,
            source_sheet[p : p + 1],
            waveform,
            electric_in[p : p + 1],
            magnetic_in[p : p + 1],
        )
        for p in range(points)
    ]
    if points == 1:
        return results[0]
    electric_out, magnetic_out, reflected, mean = (list(r) for r in zip(*results))
    return (
        jnp.concatenate(electric_out, 0),
        jnp.concatenate(magnetic_out, 0),
        jnp.concatenate(reflected, 0),
        sum(mean) / points,
    )


def solution(mesh):
    in_specs = (
        P("ka", None),
        P("sp", None, None),
        P(),
        P(),
        P("ka", None, "sp", None),
        P(),
        P("ka", None, "sp", None, None),
        P("ka", None, "sp", None, None),
    )
    out_specs = (
        P("ka", None, "sp", None, None),
        P("ka", None, "sp", None, None),
        P("ka", None),
        P(),
    )
    return jax.shard_map(
        on_device, mesh=mesh, in_specs=in_specs, out_specs=out_specs, check_vma=False
    )
```

```python
import jax
import jax.numpy as jnp
from jax import lax
from jax.experimental import pallas as pl
from jax.experimental.pallas import tpu as pltpu
from jax.sharding import PartitionSpec as P

PML = 16
INTERVAL = 5
MPHASE = 64
NMAT = 3
TIME_STEP = 0.5
MESH = pl.DeviceIdType.MESH


def rotate(couple, cosine, sine):
    return (couple[0] * cosine - couple[1] * sine, couple[0] * sine + couple[1] * cosine)


def minus(left, right):
    return (left[0] - right[0], left[1] - right[1])


def plus(left, right):
    return (left[0] + right[0], left[1] + right[1])


def relax(couple, change, keep, gain):
    return tuple(keep * c + gain * d for c, d in zip(couple, change))


def kernel(
    bloch_in,
    perm_in,
    peak_in,
    wave_in,
    material_in,
    sheet_in,
    e_hbm,
    h_hbm,
    e_ref,
    h_ref,
    power_ref,
    bloch_ref,
    perm_ref,
    peak_ref,
    wave_ref,
    material_ref,
    sheet_ref,
    e_in,
    h_in,
    report_ref,
    got_report,
    keep_ref,
    gain_ref,
    drive_ref,
    out_e,
    out_w,
    got_e,
    got_w,
    tiny,
    got_tiny,
    ahead_ref,
    send_e,
    send_w,
    recv_e,
    recv_w,
    send_tiny,
    recv_tiny,
    load_sem,
    send_report,
    recv_report,
    entered,
):
    rows, width, depth = material_ref.shape
    steps = wave_ref.shape[0]
    slabs = lax.axis_size("sp")
    slab = lax.axis_index("sp")
    upper = lax.rem(slab + 1, slabs)
    lower = lax.rem(slab + slabs - 1, slabs)

    groups = lax.axis_size("ka")
    group = lax.axis_index("ka")
    everyone = groups * slabs
    me = group * slabs + slab

    def place(at):
        return {"ka": lax.div(at, slabs), "sp": lax.rem(at, slabs)}

    last_row = rows - 1
    loads = [
        pltpu.make_async_copy(src, dst, load_sem.at[at])
        for at, (src, dst) in enumerate(
            (
                (e_hbm.at[0, :, 0], e_in.at[0, :, 0]),
                (e_hbm.at[0, :, last_row], e_in.at[0, :, last_row]),
                (h_hbm.at[0, :, last_row], h_in.at[0, :, last_row]),
                (h_hbm.at[0, :, 0], h_in.at[0, :, 0]),
                (bloch_in, bloch_ref),
                (perm_in, perm_ref),
                (peak_in, peak_ref),
                (wave_in, wave_ref),
                (e_hbm.at[0, :, 1:last_row], e_in.at[0, :, 1:last_row]),
                (h_hbm.at[0, :, 1:last_row], h_in.at[0, :, 1:last_row]),
                (material_in, material_ref),
                (sheet_in, sheet_ref),
            )
        )
    ]
    for load in loads:
        load.start()

    barrier = pltpu.get_barrier_semaphore()

    def greet(other):
        pl.semaphore_signal(barrier, inc=1, device_id=place(other), device_id_type=MESH)

    grid = groups % 4 == 0
    ahead_of = [("flip", 1), ("flip", 2)]
    stride = 1
    while stride < groups // 4 - 1:
        ahead_of.insert(0, ("line", 4 * stride))
        stride *= 2
    ahead_of = sorted(ahead_of[:-2], key=lambda turn: turn[1]) + ahead_of[-2:]
    stride = 1
    while stride < slabs // 2:
        ahead_of.append(("ring", stride))
        stride *= 2
    rounds = len(ahead_of) if grid else 0

    def peers(kind, stride):
        if kind == "flip":
            return [((group + stride * (1 - 2 * lax.rem(lax.div(group, stride), 2))) * slabs + slab, None)]
        if kind == "ring":
            return [
                (group * slabs + lax.rem(slab + stride, slabs), None),
                (group * slabs + lax.rem(slab + slabs - stride, slabs), None),
            ]
        return [
            ((group + stride) * slabs + slab, group + stride < groups),
            ((group - stride) * slabs + slab, group >= stride),
        ]

    def signal_to(semaphore, found):
        for other, exists in found:

            def signal():
                pl.semaphore_signal(
                    semaphore, inc=1, device_id=place(other), device_id_type=MESH
                )

            if exists is None:
                signal()
            else:
                pl.when(exists)(signal)

    def amount(found):
        return sum(1 if exists is None else exists.astype(jnp.int32) for _, exists in found)

    if grid:
        nearest = peers("ring", 1) + peers("flip", 1) + peers("flip", 2) + peers("line", 4)
        signal_to(barrier, nearest)
        greeted = amount(nearest)
    else:

        def greet_at(offset, carry):
            signal_to(barrier, [(lax.rem(me + offset, everyone), None)])
            return carry

        lax.fori_loop(1, everyone, greet_at, 0)
        greeted = everyone - 1

    def spread(turn):
        signal_to(entered.at[turn], peers(*ahead_of[turn]))

    def learn(turn):
        pl.semaphore_wait(entered.at[turn], amount(peers(*ahead_of[turn])))

    for load in loads[4:8]:
        load.wait()

    height = lax.broadcasted_iota(jnp.int32, (8, depth), 1).astype(jnp.float32)
    low_depth = jnp.maximum(PML - height, 0.0) / PML
    high_depth = jnp.maximum(height - (depth - 1 - PML), 0.0) / PML
    conduct = peak_ref[0] * (
        low_depth * low_depth * low_depth + high_depth * high_depth * high_depth
    )
    half_mag = conduct * (0.5 * TIME_STEP)
    h_keep = ((1.0 - half_mag) / (1.0 + half_mag))[0:1]
    h_gain = (-TIME_STEP / (1.0 + half_mag))[0:1]
    tables = []
    for level in range(NMAT):
        relative = jnp.full((8, depth), perm_ref[level], jnp.float32)
        half_ele = conduct * (0.5 * TIME_STEP) / relative
        tables.append(
            (
                ((1.0 - half_ele) / (1.0 + half_ele))[0:1],
                (TIME_STEP / relative / (1.0 + half_ele))[0:1],
            )
        )

    def trig(member):
        angle = jnp.full((8, depth), bloch_ref[0, member], jnp.int32).astype(jnp.float32)
        angle = 2.0 * jnp.pi * angle / MPHASE
        return jnp.cos(angle)[0:1], jnp.sin(angle)[0:1]

    cos_x, sin_x = trig(0)
    cos_y, sin_y = trig(1)
    at_end = (slab == slabs - 1).astype(jnp.float32)
    at_start = (slab == 0).astype(jnp.float32)
    end_cos = at_end * cos_x + (1.0 - at_end)
    end_sin = at_end * sin_x
    start_cos = at_start * cos_x + (1.0 - at_start)
    start_sin = -at_start * sin_x

    lane = lax.broadcasted_iota(jnp.int32, (width, depth), 1)
    last_lane = lane == depth - 1
    first_lane = lane == 0
    sub = lax.broadcasted_iota(jnp.int32, (8, depth), 0)

    def above_z(couple):
        return tuple(jnp.where(last_lane, 0.0, pltpu.roll(v, depth - 1, 1)) for v in couple)

    def below_z(couple):
        return tuple(jnp.where(first_lane, 0.0, pltpu.roll(v, 1, 1)) for v in couple)

    def above_y(couple):
        moved = tuple(pltpu.roll(v, width - 1, 0) for v in couple)
        tail = tuple(v[width - 8 :] for v in moved)
        turned = rotate(tail, cos_y, sin_y)
        return tuple(
            jnp.concatenate([v[: width - 8], jnp.where(sub == 7, r, w)], axis=0)
            for v, r, w in zip(moved, turned, tail)
        )

    def below_y(couple):
        moved = tuple(pltpu.roll(v, 1, 0) for v in couple)
        head = tuple(v[:8] for v in moved)
        turned = rotate(head, cos_y, -sin_y)
        return tuple(
            jnp.concatenate([jnp.where(sub == 0, r, w), v[8:]], axis=0)
            for v, r, w in zip(moved, turned, head)
        )

    def get(ref, member, x):
        return (ref[0, 2 * member, x], ref[0, 2 * member + 1, x])

    def put(ref, member, x, couple):
        ref[0, 2 * member, x] = couple[0]
        ref[0, 2 * member + 1, x] = couple[1]

    def get_plane(ref, slot, member):
        return (ref[slot, 2 * member], ref[slot, 2 * member + 1])

    def put_plane(ref, slot, member, couple):
        ref[slot, 2 * member] = couple[0]
        ref[slot, 2 * member + 1] = couple[1]

    def new_hx(x, ey, ez):
        change = minus(minus(above_y(ez), ez), minus(above_z(ey), ey))
        return relax(get(h_ref, 0, x), change, h_keep, h_gain)

    def new_hy(x, ex, ez, ez_next):
        change = minus(minus(above_z(ex), ex), minus(ez_next, ez))
        return relax(get(h_ref, 1, x), change, h_keep, h_gain)

    def new_hz(x, ex, ey, ey_next):
        change = minus(minus(ey_next, ey), minus(above_y(ex), ex))
        return relax(get(h_ref, 2, x), change, h_keep, h_gain)

    def hx_plane(x):
        put(h_ref, 0, x, new_hx(x, get(e_ref, 1, x), get(e_ref, 2, x)))

    def h_plane(x):
        ex, ey, ez = get(e_ref, 0, x), get(e_ref, 1, x), get(e_ref, 2, x)
        put(h_ref, 0, x, new_hx(x, ey, ez))
        put(h_ref, 1, x, new_hy(x, ex, ez, get(e_ref, 2, x + 1)))
        put(h_ref, 2, x, new_hz(x, ex, ey, get(e_ref, 1, x + 1)))

    def part_y(ex, ez, hy):
        return relax(hy, plus(minus(above_z(ex), ex), ez), h_keep, h_gain)

    def part_z(ex, ey, hz):
        return relax(hz, minus(minus(ex, above_y(ex)), ey), h_keep, h_gain)

    def partial_y(slot):
        x = rows - 1
        put_plane(out_w, slot, 0, part_y(get(e_ref, 0, x), get(e_ref, 2, x), get(h_ref, 1, x)))

    def partial_z(slot):
        x = rows - 1
        put_plane(out_w, slot, 1, part_z(get(e_ref, 0, x), get(e_ref, 1, x), get(h_ref, 2, x)))

    def whole_hz(slot, beyond_y):
        beyond_y = rotate(beyond_y, end_cos, end_sin)
        return tuple(w + h_gain * b for w, b in zip(get_plane(out_w, slot, 1), beyond_y))

    def whole_hy(slot, beyond_z):
        beyond_z = rotate(beyond_z, end_cos, end_sin)
        return tuple(w - h_gain * b for w, b in zip(get_plane(out_w, slot, 0), beyond_z))

    def hz_below(w_z, ey):
        turned = rotate(w_z, start_cos, start_sin)
        return tuple(w + h_gain * e for w, e in zip(turned, ey))

    def hy_below(w_y, ez):
        turned = rotate(w_y, start_cos, start_sin)
        return tuple(w - h_gain * e for w, e in zip(turned, ez))

    def new_ex(x, drive, hy, hz):
        change = minus(minus(hz, below_y(hz)), minus(hy, below_z(hy)))
        change = (change[0] - drive * drive_ref[0, x], change[1] - drive * drive_ref[1, x])
        return relax(get(e_ref, 0, x), change, keep_ref[x], gain_ref[x])

    def new_ey(x, ey, hx, hz, hz_prev):
        change = minus(minus(hx, below_z(hx)), minus(hz, hz_prev))
        return relax(ey, change, keep_ref[x], gain_ref[x])

    def new_ez(x, hx, hy, hy_prev):
        change = minus(minus(hy, hy_prev), minus(hx, below_y(hx)))
        return relax(get(e_ref, 2, x), change, keep_ref[x], gain_ref[x])

    def e_update(x, drive, hy_prev, hz_prev):
        hx, hy, hz = get(h_ref, 0, x), get(h_ref, 1, x), get(h_ref, 2, x)
        put(e_ref, 0, x, new_ex(x, drive, hy, hz))
        ey = new_ey(x, get(e_ref, 1, x), hx, hz, hz_prev)
        put(e_ref, 1, x, ey)
        ez = new_ez(x, hx, hy, hy_prev)
        put(e_ref, 2, x, ez)
        return ey, ez

    def e_middle(x, drive):
        return e_update(x, drive, get(h_ref, 1, x - 1), get(h_ref, 2, x - 1))

    def copy_e(slot, member):
        return pltpu.make_async_remote_copy(
            src_ref=out_e.at[slot, pl.ds(2 * member, 2)],
            dst_ref=got_e.at[slot, pl.ds(2 * member, 2)],
            send_sem=send_e.at[slot, member],
            recv_sem=recv_e.at[slot, member],
            device_id={"sp": lower},
            device_id_type=MESH,
        )

    def copy_w(slot, member):
        return pltpu.make_async_remote_copy(
            src_ref=out_w.at[slot, pl.ds(2 * member, 2)],
            dst_ref=got_w.at[slot, pl.ds(2 * member, 2)],
            send_sem=send_w.at[slot, member],
            recv_sem=recv_w.at[slot, member],
            device_id={"sp": upper},
            device_id_type=MESH,
        )

    square = lax.broadcasted_iota(jnp.int32, (width, width), 0) == lax.broadcasted_iota(
        jnp.int32, (width, width), 1
    )
    monitor = PML + 6
    band = monitor // 8 * 8

    def copy_tiny(at, other):
        return pltpu.make_async_remote_copy(
            src_ref=tiny.at[at],
            dst_ref=got_tiny.at[at],
            send_sem=send_tiny.at[at],
            recv_sem=recv_tiny.at[at],
            device_id={"sp": other},
            device_id_type=MESH,
        )

    def pack(at, member, couple):
        tiny[at, member] = jnp.concatenate(couple, axis=0).T[band : band + 8]

    def unpack(at, member):
        before = jnp.zeros((band, 2 * width), jnp.float32)
        after = jnp.zeros((depth - band - 8, 2 * width), jnp.float32)
        tall = jnp.concatenate([before, got_tiny[at, member], after], axis=0).T
        return tall[:width], tall[width:]

    ahead_e1, ahead_e2, ahead_e3 = (copy_tiny(at, lower) for at in range(3))
    ahead_w2, ahead_w3 = (copy_tiny(at, upper) for at in range(3, 5))

    def widen(x, carry):
        for member in range(6):
            e_ref[0, member, x] = e_in[0, member, x].astype(jnp.float32)
            h_ref[0, member, x] = h_in[0, member, x].astype(jnp.float32)
        return carry

    loads[0].wait()
    for member in range(4):
        out_e[0, member] = e_in[0, 2 + member, 0].astype(jnp.float32)
    pl.semaphore_wait(barrier, greeted)
    copy_e(0, 0).start()
    copy_e(0, 1).start()
    for load in loads[1:4]:
        load.wait()
    widen(rows - 1, 0)
    partial_z(0)
    copy_w(0, 1).start()
    partial_y(0)
    copy_w(0, 0).start()
    widen(0, 0)
    for load in loads[8:]:
        load.wait()
    lax.fori_loop(1, rows - 1, widen, 0)

    report_ref[...] = jnp.zeros_like(report_ref)

    def prepare(x, carry):
        kind = material_ref[x]
        keep, gain = tables[0]
        for level in range(1, NMAT):
            keep = jnp.where(kind == level, tables[level][0], keep)
            gain = jnp.where(kind == level, tables[level][1], gain)
        keep_ref[x] = keep
        gain_ref[x] = gain
        for part in range(2):
            row = sheet_ref[0, part, pl.ds(x, 1), :]
            column = jnp.sum(jnp.where(square, row, 0.0), axis=1, keepdims=True)
            drive_ref[part, x] = jnp.where(lane == PML + 2, column, 0.0)
        return carry

    lax.fori_loop(0, rows, prepare, 0)

    def power(x, total):
        for member in range(4):
            value = e_ref[0, member, x]
            total = total + value * value
        return total

    row_lane = lax.broadcasted_iota(jnp.int32, (1, depth), 1)
    empty = jnp.zeros((width, depth), jnp.float32)
    assert steps % (2 * INTERVAL) == 0 and rows > 6

    def note(total, at):
        amount = jnp.sum(jnp.where(lane == monitor, total, 0.0), axis=0, keepdims=True)
        amount = jnp.sum(amount, axis=1, keepdims=True)
        report_ref[...] += jnp.where(row_lane == at, amount, 0.0)

    def first_y(slot, later, sent, go):
        copy_w(slot, 1).wait_recv()
        ey = get(e_ref, 1, 0)
        hz_prev = hz_below(get_plane(got_w, slot, 1), ey)
        ey = new_ey(0, ey, get(h_ref, 0, 0), get(h_ref, 2, 0), hz_prev)
        put(e_ref, 1, 0, ey)
        if go:
            pl.when(sent)(lambda: copy_e(later, 0).wait_send())
            put_plane(out_e, later, 0, ey)
            copy_e(later, 0).start()

    def first_z(slot, later, sent, go):
        copy_w(slot, 0).wait_recv()
        hy_prev = hy_below(get_plane(got_w, slot, 0), get(e_ref, 2, 0))
        ez = new_ez(0, get(h_ref, 0, 0), get(h_ref, 1, 0), hy_prev)
        put(e_ref, 2, 0, ez)
        if go:
            pl.when(sent)(lambda: copy_e(later, 1).wait_send())
            put_plane(out_e, later, 1, ez)
            copy_e(later, 1).start()

    def first_yz_ahead(slot, later, at, copy):
        first_y(slot, later, True, False)
        first_z(slot, later, True, False)
        send_columns(at, copy)
        for member in range(2):
            copy_e(later, member).wait_send()
            put_plane(out_e, later, member, get(e_ref, 1 + member, 0))
            copy_e(later, member).start()

    def send_columns(at, copy):
        pack(at, 0, get(e_ref, 1, 0))
        pack(at, 1, get(e_ref, 2, 0))
        copy.start()

    def first_x(drive):
        put(e_ref, 0, 0, new_ex(0, drive, get(h_ref, 1, 0), get(h_ref, 2, 0)))

    def end_fields(slot, drive):
        x = rows - 1
        copy_e(slot, 0).wait_recv()
        hz = whole_hz(slot, get_plane(got_e, slot, 0))
        put(h_ref, 2, x, hz)
        hx = get(h_ref, 0, x)
        put(e_ref, 1, x, new_ey(x, get(e_ref, 1, x), hx, hz, get(h_ref, 2, x - 1)))
        copy_e(slot, 1).wait_recv()
        hy = whole_hy(slot, get_plane(got_e, slot, 1))
        put(h_ref, 1, x, hy)
        put(e_ref, 0, x, new_ex(x, drive, hy, get(h_ref, 2, x)))
        put(e_ref, 2, x, new_ez(x, get(h_ref, 0, x), hy, get(h_ref, 1, x - 1)))

    def give_w(later):
        copy_w(later, 1).wait_send()
        copy_w(later, 0).wait_send()
        partial_z(later)
        copy_w(later, 1).start()
        partial_y(later)
        copy_w(later, 0).start()

    def sides(t, slot, later, drive):
        def left():
            first_x(drive)
            ahead = t == steps - 4

            @pl.when(ahead)
            def _():
                first_yz_ahead(slot, later, 0, ahead_e1)

            @pl.when(jnp.logical_not(ahead))
            def _():
                first_y(slot, later, t >= 1, True)
                first_z(slot, later, t >= 1, True)

        def right():
            end_fields(slot, drive)

            @pl.when(t >= 1)
            def _():
                copy_w(later, 1).wait_send()
                copy_w(later, 0).wait_send()

            partial_z(later)
            copy_w(later, 1).start()
            partial_y(later)
            copy_w(later, 0).start()

        return left, right

    def before_sides():
        h_plane(0)
        h_plane(1)
        h_plane(rows - 2)
        hx_plane(rows - 1)

    def between_sides(drive):
        def both(x, held):
            e_middle(x, drive)
            h_plane(x + 1)
            return held

        lax.fori_loop(1, rows - 3, both, 0)
        e_middle(rows - 3, drive)
        e_middle(rows - 2, drive)

    def step(t, carry):
        slot = lax.rem(t, 2)
        later = lax.rem(t + 1, 2)
        drive = wave_ref[t]
        even = slot == 0
        left, right = sides(t, slot, later, drive)

        for turn in range(min(rounds, steps - 3)):

            @pl.when(t == turn)
            def _():
                if turn > 0:
                    learn(turn - 1)
                spread(turn)

        before_sides()
        pl.when(even)(right)
        pl.when(jnp.logical_not(even))(left)
        between_sides(drive)
        pl.when(even)(left)
        pl.when(jnp.logical_not(even))(right)

        @pl.when(lax.rem(t + 1, INTERVAL) == 0)
        def _():
            note(lax.fori_loop(0, rows, power, empty), lax.div(t, INTERVAL))

        return carry

    lax.fori_loop(0, steps - 3, step, 0)
    for turn in range(min(rounds, steps - 3), rounds):
        if turn > 0:
            learn(turn - 1)
        spread(turn)
    if rounds > 0:
        learn(rounds - 1)

    def tell(offset):
        return pltpu.make_async_remote_copy(
            src_ref=report_ref,
            dst_ref=got_report.at[me],
            send_sem=send_report,
            recv_sem=recv_report,
            device_id=place(lax.rem(me + offset, everyone)),
            device_id_type=MESH,
        )

    def tell_start(offset, carry):
        tell(offset).start()
        return carry

    end = rows - 1
    one, two, three = ((steps - 3 + at) % 2 for at in range(3))
    drive_one, drive, last_drive = (wave_ref[steps - 3 + at] for at in range(3))
    before_sides()
    between_sides(drive_one)
    ahead_e1.wait_recv()
    hz = whole_hz(one, unpack(0, 0))
    hy = whole_hy(one, unpack(0, 1))
    hx, hy_prev, hz_prev = get(h_ref, 0, end), get(h_ref, 1, end - 1), get(h_ref, 2, end - 1)
    ex = new_ex(end, drive_one, hy, hz)
    pack(3, 1, part_z(ex, new_ey(end, get(e_ref, 1, end), hx, hz, hz_prev), hz))
    pack(3, 0, part_y(ex, new_ez(end, hx, hy, hy_prev), hy))
    ahead_w2.start()

    first_x(drive_one)
    first_yz_ahead(one, two, 1, ahead_e2)

    h_plane(0)
    h_plane(1)

    def both(x, held):
        e_middle(x, drive)
        h_plane(x + 1)
        return held

    lax.fori_loop(1, end - 2, both, 0)
    e_middle(end - 2, drive)
    end_fields(one, drive_one)
    copy_w(two, 1).wait_send()
    copy_w(two, 0).wait_send()
    partial_z(two)
    copy_w(two, 1).start()
    partial_y(two)
    h_plane(end - 1)
    hx_plane(end)

    ahead_e2.wait_recv()
    hz = whole_hz(two, unpack(1, 0))
    hy = whole_hy(two, unpack(1, 1))
    ex = new_ex(end, drive, hy, hz)
    ey = new_ey(end, get(e_ref, 1, end), get(h_ref, 0, end), hz, get(h_ref, 2, end - 1))
    w_z = part_z(ex, ey, hz)
    pack(4, 0, w_z)
    pack(4, 1, w_z)
    ahead_w3.start()

    first_x(drive)
    ahead_w2.wait_recv()
    ey, ez = get(e_ref, 1, 0), get(e_ref, 2, 0)
    hy_prev, hz_prev = hy_below(unpack(3, 0), ez), hz_below(unpack(3, 1), ey)
    ey = new_ey(0, ey, get(h_ref, 0, 0), get(h_ref, 2, 0), hz_prev)
    ez = new_ez(0, get(h_ref, 0, 0), get(h_ref, 1, 0), hy_prev)
    put_plane(ahead_ref, 0, 0, ey)
    put_plane(ahead_ref, 0, 1, ez)
    pack(2, 0, ey)
    pack(2, 1, ez)
    ahead_e3.start()
    copy_w(two, 0).start()
    e_middle(end - 1, drive)

    h_plane(1)
    h_plane(2)

    def both_power(x, total):
        e_middle(x, last_drive)
        h_plane(x + 1)
        return power(x, total)

    total = lax.fori_loop(2, end - 2, both_power, empty)
    e_middle(end - 2, last_drive)
    total = power(end - 2, total)

    end_fields(two, drive)
    give_w(three)
    h_plane(end - 1)
    hx_plane(end)
    e_middle(end - 1, last_drive)
    total = power(end - 1, total)

    ex, ey, ez = get(e_ref, 0, 0), get_plane(ahead_ref, 0, 0), get_plane(ahead_ref, 0, 1)
    hx = new_hx(0, ey, ez)
    hy = new_hy(0, ex, ez, get(e_ref, 2, 1))
    hz = new_hz(0, ex, ey, get(e_ref, 1, 1))
    hx1, hy1, hz1 = get(h_ref, 0, 1), get(h_ref, 1, 1), get(h_ref, 2, 1)
    ahead_w3.wait_recv()
    hz_prev = hz_below(unpack(4, 1), ey)
    for value in (
        new_ex(0, last_drive, hy, hz)
        + new_ey(0, ey, hx, hz, hz_prev)
        + new_ex(1, last_drive, hy1, hz1)
        + new_ey(1, get(e_ref, 1, 1), hx1, hz1, hz)
    ):
        total = total + value * value
    ahead_e3.wait_recv()
    hx = get(h_ref, 0, end)
    hz = whole_hz(three, unpack(2, 0))
    hy = whole_hy(three, unpack(2, 1))
    for value in new_ex(end, last_drive, hy, hz) + new_ey(
        end, get(e_ref, 1, end), hx, hz, get(h_ref, 2, end - 1)
    ):
        total = total + value * value
    note(total, steps // INTERVAL - 1)
    lax.fori_loop(1, everyone, tell_start, 0)
    got_report[me] = report_ref[...]

    first_y(two, three, True, True)
    first_z(two, three, True, True)

    h_plane(0)
    e_middle(1, last_drive)
    first_x(last_drive)
    first_y(three, two, False, False)
    first_z(three, two, False, False)
    end_fields(three, last_drive)
    for at in range(2):
        for member in range(2):
            copy_e(at, member).wait_send()
            copy_w(at, member).wait_send()
    for copy in (ahead_e1, ahead_e2, ahead_e3, ahead_w2, ahead_w3):
        copy.wait_send()
    everything = got_report.at[pl.ds(0, everyone - 1)]
    pltpu.make_async_copy(everything, everything, recv_report).wait()
    pltpu.make_async_copy(everything, everything, send_report).wait()

    def gather(at, held):
        return held + got_report[group * slabs + at]

    ours = lax.fori_loop(0, slabs, gather, jnp.zeros((1, depth), jnp.float32))
    total = jnp.sum(got_report[...], axis=0)
    cells = rows * slabs * width
    power_ref[0:1] = ours / cells
    power_ref[1:2] = total / cells / groups


def write_out(e_ref, h_ref, power_ref, e_out, h_out, reflected_out, mean_out, own, mean, sems):
    members = e_ref.shape[1]
    snaps = mean.shape[0]
    writes = [
        pltpu.make_async_copy(src.at[0, member], dst.at[0, member], sems.at[at, member])
        for at, (src, dst) in enumerate(((e_ref, e_out), (h_ref, h_out)))
        for member in range(members)
    ]
    for write in writes:
        write.start()
    lane = lax.broadcasted_iota(jnp.int32, (1, power_ref.shape[1]), 1)
    for at in range(snaps):
        own[0, at] = jnp.sum(jnp.where(lane == at, power_ref[0:1], 0.0))
        mean[at] = jnp.sum(jnp.where(lane == at, power_ref[1:2], 0.0))
    small = [
        pltpu.make_async_copy(own, reflected_out, sems.at[0, members]),
        pltpu.make_async_copy(mean, mean_out, sems.at[1, members]),
    ]
    for write in small:
        write.start()
    for write in writes + small:
        write.wait()


def one_point(bloch, material, permittivity, peak, sheet, waveform, electric, magnetic):
    rows, width, depth = material.shape
    snaps = waveform.shape[0] // INTERVAL
    everyone = lax.axis_size("ka") * lax.axis_size("sp")
    hbm = pl.BlockSpec(memory_space=pltpu.HBM)
    vmem = pl.BlockSpec(memory_space=pltpu.VMEM)
    plane = (2, 4, width, depth)
    f32 = jnp.float32
    electric_end, magnetic_end, power = pl.pallas_call(
        kernel,
        out_shape=(
            jax.ShapeDtypeStruct(electric.shape, f32),
            jax.ShapeDtypeStruct(magnetic.shape, f32),
            jax.ShapeDtypeStruct((8, depth), f32),
        ),
        in_specs=[hbm] * 8,
        out_specs=(vmem, vmem, vmem),
        scratch_shapes=[
            pltpu.SMEM(bloch.shape, jnp.int32),
            pltpu.SMEM(permittivity.shape, f32),
            pltpu.SMEM(peak.shape, f32),
            pltpu.SMEM(waveform.shape, f32),
            pltpu.VMEM(material.shape, jnp.int32),
            pltpu.VMEM(sheet.shape, f32),
            pltpu.VMEM(electric.shape, electric.dtype),
            pltpu.VMEM(magnetic.shape, magnetic.dtype),
            pltpu.VMEM((1, depth), f32),
            pltpu.VMEM((everyone, 1, depth), f32),
            pltpu.VMEM((rows, width, depth), f32),
            pltpu.VMEM((rows, width, depth), f32),
            pltpu.VMEM((2, rows, width, depth), f32),
            pltpu.VMEM(plane, f32),
            pltpu.VMEM(plane, f32),
            pltpu.VMEM(plane, f32),
            pltpu.VMEM(plane, f32),
            pltpu.VMEM((5, 2, 8, 2 * width), f32),
            pltpu.VMEM((5, 2, 8, 2 * width), f32),
            pltpu.VMEM((1, 4, width, depth), f32),
            pltpu.SemaphoreType.DMA((2, 2)),
            pltpu.SemaphoreType.DMA((2, 2)),
            pltpu.SemaphoreType.DMA((2, 2)),
            pltpu.SemaphoreType.DMA((2, 2)),
            pltpu.SemaphoreType.DMA((5,)),
            pltpu.SemaphoreType.DMA((5,)),
            pltpu.SemaphoreType.DMA((12,)),
            pltpu.SemaphoreType.DMA,
            pltpu.SemaphoreType.DMA,
            pltpu.SemaphoreType.REGULAR((2 + everyone.bit_length(),)),
        ],
        compiler_params=pltpu.CompilerParams(
            collective_id=0, has_side_effects=True, vmem_limit_bytes=40 * 1024 * 1024
        ),
    )(*((v if v.shape == (1,) else pltpu.with_memory_space_constraint(v, pltpu.HBM)) for v in (bloch, permittivity, peak, waveform, material, sheet, electric, magnetic)))
    return pl.pallas_call(
        write_out,
        out_shape=(
            pltpu.HBM(electric.shape, f32),
            pltpu.HBM(magnetic.shape, f32),
            pltpu.HBM((1, snaps), f32),
            pltpu.HBM((snaps,), f32),
        ),
        in_specs=[vmem] * 3,
        out_specs=(hbm,) * 4,
        scratch_shapes=[
            pltpu.SMEM((1, snaps), f32),
            pltpu.SMEM((snaps,), f32),
            pltpu.SemaphoreType.DMA((2, electric.shape[1] + 1)),
        ],
        compiler_params=pltpu.CompilerParams(vmem_limit_bytes=1024 * 1024),
    )(electric_end, magnetic_end, power)


def on_device(
    bloch_index,
    material,
    permittivity,
    absorption_peak,
    source_sheet,
    waveform,
    electric_in,
    magnetic_in,
):
    points = bloch_index.shape[0]
    results = [
        one_point(
            bloch_index[p : p + 1],
            material,
            permittivity,
            absorption_peak,
            source_sheet[p : p + 1],
            waveform,
            electric_in[p : p + 1],
            magnetic_in[p : p + 1],
        )
        for p in range(points)
    ]
    if points == 1:
        return results[0]
    electric_out, magnetic_out, reflected, mean = (list(r) for r in zip(*results))
    return (
        jnp.concatenate(electric_out, 0),
        jnp.concatenate(magnetic_out, 0),
        jnp.concatenate(reflected, 0),
        sum(mean) / points,
    )


def solution(mesh):
    in_specs = (
        P("ka", None),
        P("sp", None, None),
        P(),
        P(),
        P("ka", None, "sp", None),
        P(),
        P("ka", None, "sp", None, None),
        P("ka", None, "sp", None, None),
    )
    out_specs = (
        P("ka", None, "sp", None, None),
        P("ka", None, "sp", None, None),
        P("ka", None),
        P(),
    )
    return jax.shard_map(
        on_device, mesh=mesh, in_specs=in_specs, out_specs=out_specs, check_vma=False
    )
```

```python
import jax
import jax.numpy as jnp
from jax import lax
from jax.experimental import pallas as pl
from jax.experimental.pallas import tpu as pltpu
from jax.sharding import PartitionSpec as P

PML = 16
INTERVAL = 5
MPHASE = 64
NMAT = 3
TIME_STEP = 0.5
MESH = pl.DeviceIdType.MESH


def rotate(couple, cosine, sine):
    return (couple[0] * cosine - couple[1] * sine, couple[0] * sine + couple[1] * cosine)


def minus(left, right):
    return (left[0] - right[0], left[1] - right[1])


def plus(left, right):
    return (left[0] + right[0], left[1] + right[1])


def relax(couple, change, keep, gain):
    return tuple(keep * c + gain * d for c, d in zip(couple, change))


def kernel(
    bloch_in,
    perm_in,
    peak_in,
    wave_in,
    material_in,
    sheet_in,
    e_hbm,
    h_hbm,
    e_ref,
    h_ref,
    power_ref,
    bloch_ref,
    perm_ref,
    peak_ref,
    wave_ref,
    material_ref,
    sheet_ref,
    e_in,
    h_in,
    report_ref,
    got_report,
    keep_ref,
    gain_ref,
    drive_ref,
    out_e,
    out_w,
    got_e,
    got_w,
    tiny,
    got_tiny,
    ahead_ref,
    send_e,
    send_w,
    recv_e,
    recv_w,
    send_tiny,
    recv_tiny,
    load_sem,
    send_report,
    recv_report,
    entered,
):
    rows, width, depth = material_ref.shape
    steps = wave_ref.shape[0]
    slabs = lax.axis_size("sp")
    slab = lax.axis_index("sp")
    upper = lax.rem(slab + 1, slabs)
    lower = lax.rem(slab + slabs - 1, slabs)

    groups = lax.axis_size("ka")
    group = lax.axis_index("ka")
    everyone = groups * slabs
    me = group * slabs + slab

    def place(at):
        return {"ka": lax.div(at, slabs), "sp": lax.rem(at, slabs)}

    barrier = pltpu.get_barrier_semaphore()

    def greet(other):
        pl.semaphore_signal(barrier, inc=1, device_id=place(other), device_id_type=MESH)

    grid = groups % 4 == 0
    ahead_of = [("flip", 1), ("flip", 2)]
    stride = 1
    while stride < groups // 4 - 1:
        ahead_of.insert(0, ("line", 4 * stride))
        stride *= 2
    ahead_of = sorted(ahead_of[:-2], key=lambda turn: turn[1]) + ahead_of[-2:]
    stride = 1
    while stride < slabs // 2:
        ahead_of.append(("ring", stride))
        stride *= 2
    rounds = len(ahead_of) if grid else 0

    def peers(kind, stride):
        if kind == "flip":
            return [((group + stride * (1 - 2 * lax.rem(lax.div(group, stride), 2))) * slabs + slab, None)]
        if kind == "ring":
            return [
                (group * slabs + lax.rem(slab + stride, slabs), None),
                (group * slabs + lax.rem(slab + slabs - stride, slabs), None),
            ]
        return [
            ((group + stride) * slabs + slab, group + stride < groups),
            ((group - stride) * slabs + slab, group >= stride),
        ]

    def signal_to(semaphore, found):
        for other, exists in found:

            def signal():
                pl.semaphore_signal(
                    semaphore, inc=1, device_id=place(other), device_id_type=MESH
                )

            if exists is None:
                signal()
            else:
                pl.when(exists)(signal)

    def amount(found):
        return sum(1 if exists is None else exists.astype(jnp.int32) for _, exists in found)

    if grid:
        nearest = peers("ring", 1) + peers("flip", 1) + peers("flip", 2) + peers("line", 4)
        signal_to(barrier, nearest)
        greeted = amount(nearest)
    else:

        def greet_at(offset, carry):
            signal_to(barrier, [(lax.rem(me + offset, everyone), None)])
            return carry

        lax.fori_loop(1, everyone, greet_at, 0)
        greeted = everyone - 1

    def spread(turn):
        signal_to(entered.at[turn], peers(*ahead_of[turn]))

    def learn(turn):
        pl.semaphore_wait(entered.at[turn], amount(peers(*ahead_of[turn])))

    last_row = rows - 1
    loads = [
        pltpu.make_async_copy(src, dst, load_sem.at[at])
        for at, (src, dst) in enumerate(
            (
                (e_hbm.at[0, pl.ds(2, 4), 0], e_in.at[0, pl.ds(2, 4), 0]),
                (e_hbm.at[0, :, last_row], e_in.at[0, :, last_row]),
                (h_hbm.at[0, :, last_row], h_in.at[0, :, last_row]),
                (h_hbm.at[0, :, 0], h_in.at[0, :, 0]),
                (e_hbm.at[0, pl.ds(0, 2), 0], e_in.at[0, pl.ds(0, 2), 0]),
                (bloch_in, bloch_ref),
                (perm_in, perm_ref),
                (peak_in, peak_ref),
                (wave_in, wave_ref),
                (e_hbm.at[0, :, 1:last_row], e_in.at[0, :, 1:last_row]),
                (h_hbm.at[0, :, 1:last_row], h_in.at[0, :, 1:last_row]),
                (material_in, material_ref),
                (sheet_in, sheet_ref),
            )
        )
    ]
    for load in loads:
        load.start()

    def copy_e(slot, member):
        return pltpu.make_async_remote_copy(
            src_ref=out_e.at[slot, pl.ds(2 * member, 2)],
            dst_ref=got_e.at[slot, pl.ds(2 * member, 2)],
            send_sem=send_e.at[slot, member],
            recv_sem=recv_e.at[slot, member],
            device_id={"sp": lower},
            device_id_type=MESH,
        )

    loads[0].wait()
    for member in range(4):
        out_e[0, member] = e_in[0, 2 + member, 0].astype(jnp.float32)
    pl.semaphore_wait(barrier, greeted)
    copy_e(0, 0).start()
    copy_e(0, 1).start()
    for load in loads[5:9]:
        load.wait()

    height = lax.broadcasted_iota(jnp.int32, (8, depth), 1).astype(jnp.float32)
    low_depth = jnp.maximum(PML - height, 0.0) / PML
    high_depth = jnp.maximum(height - (depth - 1 - PML), 0.0) / PML
    conduct = peak_ref[0] * (
        low_depth * low_depth * low_depth + high_depth * high_depth * high_depth
    )
    half_mag = conduct * (0.5 * TIME_STEP)
    h_keep = ((1.0 - half_mag) / (1.0 + half_mag))[0:1]
    h_gain = (-TIME_STEP / (1.0 + half_mag))[0:1]
    tables = []
    for level in range(NMAT):
        relative = jnp.full((8, depth), perm_ref[level], jnp.float32)
        half_ele = conduct * (0.5 * TIME_STEP) / relative
        tables.append(
            (
                ((1.0 - half_ele) / (1.0 + half_ele))[0:1],
                (TIME_STEP / relative / (1.0 + half_ele))[0:1],
            )
        )

    def trig(member):
        angle = jnp.full((8, depth), bloch_ref[0, member], jnp.int32).astype(jnp.float32)
        angle = 2.0 * jnp.pi * angle / MPHASE
        return jnp.cos(angle)[0:1], jnp.sin(angle)[0:1]

    cos_x, sin_x = trig(0)
    cos_y, sin_y = trig(1)
    at_end = (slab == slabs - 1).astype(jnp.float32)
    at_start = (slab == 0).astype(jnp.float32)
    end_cos = at_end * cos_x + (1.0 - at_end)
    end_sin = at_end * sin_x
    start_cos = at_start * cos_x + (1.0 - at_start)
    start_sin = -at_start * sin_x

    lane = lax.broadcasted_iota(jnp.int32, (width, depth), 1)
    last_lane = lane == depth - 1
    first_lane = lane == 0
    sub = lax.broadcasted_iota(jnp.int32, (8, depth), 0)

    def above_z(couple):
        return tuple(jnp.where(last_lane, 0.0, pltpu.roll(v, depth - 1, 1)) for v in couple)

    def below_z(couple):
        return tuple(jnp.where(first_lane, 0.0, pltpu.roll(v, 1, 1)) for v in couple)

    def above_y(couple):
        moved = tuple(pltpu.roll(v, width - 1, 0) for v in couple)
        tail = tuple(v[width - 8 :] for v in moved)
        turned = rotate(tail, cos_y, sin_y)
        return tuple(
            jnp.concatenate([v[: width - 8], jnp.where(sub == 7, r, w)], axis=0)
            for v, r, w in zip(moved, turned, tail)
        )

    def below_y(couple):
        moved = tuple(pltpu.roll(v, 1, 0) for v in couple)
        head = tuple(v[:8] for v in moved)
        turned = rotate(head, cos_y, -sin_y)
        return tuple(
            jnp.concatenate([jnp.where(sub == 0, r, w), v[8:]], axis=0)
            for v, r, w in zip(moved, turned, head)
        )

    def get(ref, member, x):
        return (ref[0, 2 * member, x], ref[0, 2 * member + 1, x])

    def put(ref, member, x, couple):
        ref[0, 2 * member, x] = couple[0]
        ref[0, 2 * member + 1, x] = couple[1]

    def get_plane(ref, slot, member):
        return (ref[slot, 2 * member], ref[slot, 2 * member + 1])

    def put_plane(ref, slot, member, couple):
        ref[slot, 2 * member] = couple[0]
        ref[slot, 2 * member + 1] = couple[1]

    def new_hx(x, ey, ez):
        change = minus(minus(above_y(ez), ez), minus(above_z(ey), ey))
        return relax(get(h_ref, 0, x), change, h_keep, h_gain)

    def new_hy(x, ex, ez, ez_next):
        change = minus(minus(above_z(ex), ex), minus(ez_next, ez))
        return relax(get(h_ref, 1, x), change, h_keep, h_gain)

    def new_hz(x, ex, ey, ey_next):
        change = minus(minus(ey_next, ey), minus(above_y(ex), ex))
        return relax(get(h_ref, 2, x), change, h_keep, h_gain)

    def hx_plane(x):
        put(h_ref, 0, x, new_hx(x, get(e_ref, 1, x), get(e_ref, 2, x)))

    def h_plane(x):
        ex, ey, ez = get(e_ref, 0, x), get(e_ref, 1, x), get(e_ref, 2, x)
        put(h_ref, 0, x, new_hx(x, ey, ez))
        put(h_ref, 1, x, new_hy(x, ex, ez, get(e_ref, 2, x + 1)))
        put(h_ref, 2, x, new_hz(x, ex, ey, get(e_ref, 1, x + 1)))

    def part_y(ex, ez, hy):
        return relax(hy, plus(minus(above_z(ex), ex), ez), h_keep, h_gain)

    def part_z(ex, ey, hz):
        return relax(hz, minus(minus(ex, above_y(ex)), ey), h_keep, h_gain)

    def partial_y(slot):
        x = rows - 1
        put_plane(out_w, slot, 0, part_y(get(e_ref, 0, x), get(e_ref, 2, x), get(h_ref, 1, x)))

    def partial_z(slot):
        x = rows - 1
        put_plane(out_w, slot, 1, part_z(get(e_ref, 0, x), get(e_ref, 1, x), get(h_ref, 2, x)))

    def whole_hz(slot, beyond_y):
        beyond_y = rotate(beyond_y, end_cos, end_sin)
        return tuple(w + h_gain * b for w, b in zip(get_plane(out_w, slot, 1), beyond_y))

    def whole_hy(slot, beyond_z):
        beyond_z = rotate(beyond_z, end_cos, end_sin)
        return tuple(w - h_gain * b for w, b in zip(get_plane(out_w, slot, 0), beyond_z))

    def hz_below(w_z, ey):
        turned = rotate(w_z, start_cos, start_sin)
        return tuple(w + h_gain * e for w, e in zip(turned, ey))

    def hy_below(w_y, ez):
        turned = rotate(w_y, start_cos, start_sin)
        return tuple(w - h_gain * e for w, e in zip(turned, ez))

    def new_ex(x, drive, hy, hz):
        change = minus(minus(hz, below_y(hz)), minus(hy, below_z(hy)))
        change = (change[0] - drive * drive_ref[0, x], change[1] - drive * drive_ref[1, x])
        return relax(get(e_ref, 0, x), change, keep_ref[x], gain_ref[x])

    def new_ey(x, ey, hx, hz, hz_prev):
        change = minus(minus(hx, below_z(hx)), minus(hz, hz_prev))
        return relax(ey, change, keep_ref[x], gain_ref[x])

    def new_ez(x, hx, hy, hy_prev):
        change = minus(minus(hy, hy_prev), minus(hx, below_y(hx)))
        return relax(get(e_ref, 2, x), change, keep_ref[x], gain_ref[x])

    def e_update(x, drive, hy_prev, hz_prev):
        hx, hy, hz = get(h_ref, 0, x), get(h_ref, 1, x), get(h_ref, 2, x)
        put(e_ref, 0, x, new_ex(x, drive, hy, hz))
        ey = new_ey(x, get(e_ref, 1, x), hx, hz, hz_prev)
        put(e_ref, 1, x, ey)
        ez = new_ez(x, hx, hy, hy_prev)
        put(e_ref, 2, x, ez)
        return ey, ez

    def e_middle_xy(x, drive):
        hx, hy, hz = get(h_ref, 0, x), get(h_ref, 1, x), get(h_ref, 2, x)
        put(e_ref, 0, x, new_ex(x, drive, hy, hz))
        put(e_ref, 1, x, new_ey(x, get(e_ref, 1, x), hx, hz, get(h_ref, 2, x - 1)))

    def e_middle_z(x, carry):
        hx, hy = get(h_ref, 0, x), get(h_ref, 1, x)
        put(e_ref, 2, x, new_ez(x, hx, hy, get(h_ref, 1, x - 1)))
        return carry

    def e_middle(x, drive):
        return e_update(x, drive, get(h_ref, 1, x - 1), get(h_ref, 2, x - 1))

    def copy_w(slot, member):
        return pltpu.make_async_remote_copy(
            src_ref=out_w.at[slot, pl.ds(2 * member, 2)],
            dst_ref=got_w.at[slot, pl.ds(2 * member, 2)],
            send_sem=send_w.at[slot, member],
            recv_sem=recv_w.at[slot, member],
            device_id={"sp": upper},
            device_id_type=MESH,
        )

    square = lax.broadcasted_iota(jnp.int32, (width, width), 0) == lax.broadcasted_iota(
        jnp.int32, (width, width), 1
    )
    monitor = PML + 6
    band = monitor // 8 * 8

    def copy_tiny(at, other):
        return pltpu.make_async_remote_copy(
            src_ref=tiny.at[at],
            dst_ref=got_tiny.at[at],
            send_sem=send_tiny.at[at],
            recv_sem=recv_tiny.at[at],
            device_id={"sp": other},
            device_id_type=MESH,
        )

    def pack(at, member, couple):
        tiny[at, member] = jnp.concatenate(couple, axis=0).T[band : band + 8]

    def unpack(at, member):
        before = jnp.zeros((band, 2 * width), jnp.float32)
        after = jnp.zeros((depth - band - 8, 2 * width), jnp.float32)
        tall = jnp.concatenate([before, got_tiny[at, member], after], axis=0).T
        return tall[:width], tall[width:]

    ahead_e1, ahead_e2, ahead_e3 = (copy_tiny(at, lower) for at in range(3))
    ahead_w2, ahead_w3 = (copy_tiny(at, upper) for at in range(3, 5))

    def widen(x, carry):
        for member in range(6):
            e_ref[0, member, x] = e_in[0, member, x].astype(jnp.float32)
            h_ref[0, member, x] = h_in[0, member, x].astype(jnp.float32)
        return carry

    for load in loads[1:5]:
        load.wait()
    widen(rows - 1, 0)
    partial_z(0)
    copy_w(0, 1).start()
    partial_y(0)
    copy_w(0, 0).start()
    widen(0, 0)
    for load in loads[9:]:
        load.wait()
    lax.fori_loop(1, rows - 1, widen, 0)

    report_ref[...] = jnp.zeros_like(report_ref)

    def prepare(x, carry):
        kind = material_ref[x]
        keep, gain = tables[0]
        for level in range(1, NMAT):
            keep = jnp.where(kind == level, tables[level][0], keep)
            gain = jnp.where(kind == level, tables[level][1], gain)
        keep_ref[x] = keep
        gain_ref[x] = gain
        for part in range(2):
            row = sheet_ref[0, part, pl.ds(x, 1), :]
            column = jnp.sum(jnp.where(square, row, 0.0), axis=1, keepdims=True)
            drive_ref[part, x] = jnp.where(lane == PML + 2, column, 0.0)
        return carry

    together = 4 if rows % 4 == 0 else 1

    def prepare_some(group_of, carry):
        for at in range(together):
            prepare(group_of * together + at, carry)
        return carry

    lax.fori_loop(0, rows // together, prepare_some, 0)

    def power(x, total):
        for member in range(4):
            value = e_ref[0, member, x]
            total = total + value * value
        return total

    empty = jnp.zeros((width, depth), jnp.float32)
    assert steps % (2 * INTERVAL) == 0 and rows > 6

    def note(total, at):
        report_ref[pl.ds(at, 1)] = jnp.sum(total, axis=0, keepdims=True)

    def first_y(slot, later, sent, go):
        copy_w(slot, 1).wait_recv()
        ey = get(e_ref, 1, 0)
        hz_prev = hz_below(get_plane(got_w, slot, 1), ey)
        ey = new_ey(0, ey, get(h_ref, 0, 0), get(h_ref, 2, 0), hz_prev)
        put(e_ref, 1, 0, ey)
        if go:
            pl.when(sent)(lambda: copy_e(later, 0).wait_send())
            put_plane(out_e, later, 0, ey)
            copy_e(later, 0).start()

    def first_z(slot, later, sent, go):
        copy_w(slot, 0).wait_recv()
        hy_prev = hy_below(get_plane(got_w, slot, 0), get(e_ref, 2, 0))
        ez = new_ez(0, get(h_ref, 0, 0), get(h_ref, 1, 0), hy_prev)
        put(e_ref, 2, 0, ez)
        if go:
            pl.when(sent)(lambda: copy_e(later, 1).wait_send())
            put_plane(out_e, later, 1, ez)
            copy_e(later, 1).start()

    def first_yz_ahead(slot, later, at, copy):
        first_y(slot, later, True, False)
        first_z(slot, later, True, False)
        send_columns(at, copy)
        for member in range(2):
            copy_e(later, member).wait_send()
            put_plane(out_e, later, member, get(e_ref, 1 + member, 0))
            copy_e(later, member).start()

    def send_columns(at, copy):
        pack(at, 0, get(e_ref, 1, 0))
        pack(at, 1, get(e_ref, 2, 0))
        copy.start()

    def first_x(drive):
        put(e_ref, 0, 0, new_ex(0, drive, get(h_ref, 1, 0), get(h_ref, 2, 0)))

    def end_fields(slot, drive):
        x = rows - 1
        copy_e(slot, 0).wait_recv()
        hz = whole_hz(slot, get_plane(got_e, slot, 0))
        put(h_ref, 2, x, hz)
        hx = get(h_ref, 0, x)
        put(e_ref, 1, x, new_ey(x, get(e_ref, 1, x), hx, hz, get(h_ref, 2, x - 1)))
        copy_e(slot, 1).wait_recv()
        hy = whole_hy(slot, get_plane(got_e, slot, 1))
        put(h_ref, 1, x, hy)
        put(e_ref, 0, x, new_ex(x, drive, hy, get(h_ref, 2, x)))
        put(e_ref, 2, x, new_ez(x, get(h_ref, 0, x), hy, get(h_ref, 1, x - 1)))

    def give_w(later):
        copy_w(later, 1).wait_send()
        copy_w(later, 0).wait_send()
        partial_z(later)
        copy_w(later, 1).start()
        partial_y(later)
        copy_w(later, 0).start()

    def sides(t, slot, later, drive):
        def left():
            first_x(drive)
            ahead = t == steps - 4

            @pl.when(ahead)
            def _():
                first_yz_ahead(slot, later, 0, ahead_e1)

            @pl.when(jnp.logical_not(ahead))
            def _():
                first_y(slot, later, t >= 1, True)
                first_z(slot, later, t >= 1, True)

        def right():
            end_fields(slot, drive)

            @pl.when(t >= 1)
            def _():
                copy_w(later, 1).wait_send()
                copy_w(later, 0).wait_send()

            partial_z(later)
            copy_w(later, 1).start()
            partial_y(later)
            copy_w(later, 0).start()

        return left, right

    def before_sides():
        h_plane(0)
        h_plane(1)
        h_plane(rows - 2)
        hx_plane(rows - 1)

    def between_sides(drive):
        def both(x, held):
            e_middle(x, drive)
            h_plane(x + 1)
            return held

        lax.fori_loop(1, rows - 3, both, 0)
        e_middle(rows - 3, drive)
        e_middle(rows - 2, drive)

    def step(t, carry):
        slot = lax.rem(t, 2)
        later = lax.rem(t + 1, 2)
        drive = wave_ref[t]
        even = slot == 0
        left, right = sides(t, slot, later, drive)

        for turn in range(min(rounds, steps - 3)):

            @pl.when(t == turn)
            def _():
                if turn > 0:
                    learn(turn - 1)
                spread(turn)

        before_sides()
        pl.when(even)(right)
        pl.when(jnp.logical_not(even))(left)
        between_sides(drive)
        pl.when(even)(left)
        pl.when(jnp.logical_not(even))(right)

        @pl.when(lax.rem(t + 1, INTERVAL) == 0)
        def _():
            note(lax.fori_loop(0, rows, power, empty), lax.div(t, INTERVAL))

        return carry

    lax.fori_loop(0, steps - 3, step, 0)
    for turn in range(min(rounds, steps - 3), rounds):
        if turn > 0:
            learn(turn - 1)
        spread(turn)
    if rounds > 0:
        learn(rounds - 1)

    def tell(offset):
        return pltpu.make_async_remote_copy(
            src_ref=report_ref,
            dst_ref=got_report.at[me],
            send_sem=send_report,
            recv_sem=recv_report,
            device_id=place(lax.rem(me + offset, everyone)),
            device_id_type=MESH,
        )

    def tell_start(offset, carry):
        tell(offset).start()
        return carry

    end = rows - 1
    one, two, three = ((steps - 3 + at) % 2 for at in range(3))
    drive_one, drive, last_drive = (wave_ref[steps - 3 + at] for at in range(3))
    before_sides()
    between_sides(drive_one)
    ahead_e1.wait_recv()
    hz = whole_hz(one, unpack(0, 0))
    hy = whole_hy(one, unpack(0, 1))
    hx, hy_prev, hz_prev = get(h_ref, 0, end), get(h_ref, 1, end - 1), get(h_ref, 2, end - 1)
    ex = new_ex(end, drive_one, hy, hz)
    pack(3, 1, part_z(ex, new_ey(end, get(e_ref, 1, end), hx, hz, hz_prev), hz))
    pack(3, 0, part_y(ex, new_ez(end, hx, hy, hy_prev), hy))
    ahead_w2.start()

    first_x(drive_one)
    first_yz_ahead(one, two, 1, ahead_e2)

    h_plane(0)
    h_plane(1)

    def both(x, held):
        e_middle(x, drive)
        h_plane(x + 1)
        return held

    lax.fori_loop(1, end - 2, both, 0)
    e_middle(end - 2, drive)
    end_fields(one, drive_one)
    copy_w(two, 1).wait_send()
    copy_w(two, 0).wait_send()
    partial_z(two)
    copy_w(two, 1).start()
    partial_y(two)
    h_plane(end - 1)
    hx_plane(end)

    ahead_e2.wait_recv()
    hz = whole_hz(two, unpack(1, 0))
    hy = whole_hy(two, unpack(1, 1))
    ex = new_ex(end, drive, hy, hz)
    ey = new_ey(end, get(e_ref, 1, end), get(h_ref, 0, end), hz, get(h_ref, 2, end - 1))
    w_z = part_z(ex, ey, hz)
    pack(4, 0, w_z)
    pack(4, 1, w_z)
    ahead_w3.start()

    first_x(drive)
    ahead_w2.wait_recv()
    ey, ez = get(e_ref, 1, 0), get(e_ref, 2, 0)
    hy_prev, hz_prev = hy_below(unpack(3, 0), ez), hz_below(unpack(3, 1), ey)
    ey = new_ey(0, ey, get(h_ref, 0, 0), get(h_ref, 2, 0), hz_prev)
    ez = new_ez(0, get(h_ref, 0, 0), get(h_ref, 1, 0), hy_prev)
    put_plane(ahead_ref, 0, 0, ey)
    put_plane(ahead_ref, 0, 1, ez)
    pack(2, 0, ey)
    pack(2, 1, ez)
    ahead_e3.start()
    copy_w(two, 0).start()
    e_middle(end - 1, drive)

    h_plane(1)
    h_plane(2)

    def both_power(x, total):
        e_middle_xy(x, last_drive)
        h_plane(x + 1)
        return power(x, total)

    total = lax.fori_loop(2, end - 2, both_power, empty)
    e_middle_xy(end - 2, last_drive)
    total = power(end - 2, total)

    end_fields(two, drive)
    give_w(three)
    h_plane(end - 1)
    hx_plane(end)
    e_middle_xy(end - 1, last_drive)
    total = power(end - 1, total)

    ex, ey, ez = get(e_ref, 0, 0), get_plane(ahead_ref, 0, 0), get_plane(ahead_ref, 0, 1)
    hx = new_hx(0, ey, ez)
    hy = new_hy(0, ex, ez, get(e_ref, 2, 1))
    hz = new_hz(0, ex, ey, get(e_ref, 1, 1))
    hx1, hy1, hz1 = get(h_ref, 0, 1), get(h_ref, 1, 1), get(h_ref, 2, 1)
    ahead_w3.wait_recv()
    hz_prev = hz_below(unpack(4, 1), ey)
    for value in (
        new_ex(0, last_drive, hy, hz)
        + new_ey(0, ey, hx, hz, hz_prev)
        + new_ex(1, last_drive, hy1, hz1)
        + new_ey(1, get(e_ref, 1, 1), hx1, hz1, hz)
    ):
        total = total + value * value
    ahead_e3.wait_recv()
    hx = get(h_ref, 0, end)
    hz = whole_hz(three, unpack(2, 0))
    hy = whole_hy(three, unpack(2, 1))
    for value in new_ex(end, last_drive, hy, hz) + new_ey(
        end, get(e_ref, 1, end), hx, hz, get(h_ref, 2, end - 1)
    ):
        total = total + value * value
    note(total, steps // INTERVAL - 1)
    lax.fori_loop(1, everyone, tell_start, 0)
    got_report[me] = report_ref[...]

    first_y(two, three, True, True)
    first_z(two, three, True, True)

    lax.fori_loop(2, end, e_middle_z, 0)
    h_plane(0)
    e_middle(1, last_drive)
    first_x(last_drive)
    first_y(three, two, False, False)
    first_z(three, two, False, False)
    end_fields(three, last_drive)
    for at in range(2):
        for member in range(2):
            copy_e(at, member).wait_send()
            copy_w(at, member).wait_send()
    for copy in (ahead_e1, ahead_e2, ahead_e3, ahead_w2, ahead_w3):
        copy.wait_send()
    everything = got_report.at[pl.ds(0, everyone - 1)]
    pltpu.make_async_copy(everything, everything, recv_report).wait()
    pltpu.make_async_copy(everything, everything, send_report).wait()

    def gather(at, held):
        return held + got_report[group * slabs + at]

    ours = lax.fori_loop(0, slabs, gather, jnp.zeros(report_ref.shape, jnp.float32))
    total = jnp.sum(got_report[...], axis=0)
    cells = rows * slabs * width
    power_ref[0] = ours / cells
    power_ref[1] = total / cells / groups


def write_out(e_ref, h_ref, power_ref, e_out, h_out, reflected_out, mean_out, own, mean, sems):
    members = e_ref.shape[1]
    snaps = mean.shape[0]
    writes = [
        pltpu.make_async_copy(src.at[0, member], dst.at[0, member], sems.at[at, member])
        for at, (src, dst) in enumerate(((e_ref, e_out), (h_ref, h_out)))
        for member in range(members)
    ]
    for write in writes:
        write.start()
    lane = lax.broadcasted_iota(jnp.int32, (1, power_ref.shape[2]), 1)
    chosen = lane == PML + 6
    for at in range(snaps):
        own[0, at] = jnp.sum(jnp.where(chosen, power_ref[0, at : at + 1], 0.0))
        mean[at] = jnp.sum(jnp.where(chosen, power_ref[1, at : at + 1], 0.0))
    small = [
        pltpu.make_async_copy(own, reflected_out, sems.at[0, members]),
        pltpu.make_async_copy(mean, mean_out, sems.at[1, members]),
    ]
    for write in small:
        write.start()
    for write in writes + small:
        write.wait()


def one_point(bloch, material, permittivity, peak, sheet, waveform, electric, magnetic):
    rows, width, depth = material.shape
    snaps = waveform.shape[0] // INTERVAL
    everyone = lax.axis_size("ka") * lax.axis_size("sp")
    hbm = pl.BlockSpec(memory_space=pltpu.HBM)
    vmem = pl.BlockSpec(memory_space=pltpu.VMEM)
    plane = (2, 4, width, depth)
    f32 = jnp.float32
    electric_end, magnetic_end, power = pl.pallas_call(
        kernel,
        out_shape=(
            jax.ShapeDtypeStruct(electric.shape, f32),
            jax.ShapeDtypeStruct(magnetic.shape, f32),
            jax.ShapeDtypeStruct((2, snaps, depth), f32),
        ),
        in_specs=[hbm] * 8,
        out_specs=(vmem, vmem, vmem),
        scratch_shapes=[
            pltpu.SMEM(bloch.shape, jnp.int32),
            pltpu.SMEM(permittivity.shape, f32),
            pltpu.SMEM(peak.shape, f32),
            pltpu.SMEM(waveform.shape, f32),
            pltpu.VMEM(material.shape, jnp.int32),
            pltpu.VMEM(sheet.shape, f32),
            pltpu.VMEM(electric.shape, electric.dtype),
            pltpu.VMEM(magnetic.shape, magnetic.dtype),
            pltpu.VMEM((snaps, depth), f32),
            pltpu.VMEM((everyone, snaps, depth), f32),
            pltpu.VMEM((rows, width, depth), f32),
            pltpu.VMEM((rows, width, depth), f32),
            pltpu.VMEM((2, rows, width, depth), f32),
            pltpu.VMEM(plane, f32),
            pltpu.VMEM(plane, f32),
            pltpu.VMEM(plane, f32),
            pltpu.VMEM(plane, f32),
            pltpu.VMEM((5, 2, 8, 2 * width), f32),
            pltpu.VMEM((5, 2, 8, 2 * width), f32),
            pltpu.VMEM((1, 4, width, depth), f32),
            pltpu.SemaphoreType.DMA((2, 2)),
            pltpu.SemaphoreType.DMA((2, 2)),
            pltpu.SemaphoreType.DMA((2, 2)),
            pltpu.SemaphoreType.DMA((2, 2)),
            pltpu.SemaphoreType.DMA((5,)),
            pltpu.SemaphoreType.DMA((5,)),
            pltpu.SemaphoreType.DMA((13,)),
            pltpu.SemaphoreType.DMA,
            pltpu.SemaphoreType.DMA,
            pltpu.SemaphoreType.REGULAR((2 + everyone.bit_length(),)),
        ],
        compiler_params=pltpu.CompilerParams(
            collective_id=0, has_side_effects=True, vmem_limit_bytes=40 * 1024 * 1024
        ),
    )(*((v if v.shape == (1,) else pltpu.with_memory_space_constraint(v, pltpu.HBM)) for v in (bloch, permittivity, peak, waveform, material, sheet, electric, magnetic)))
    return pl.pallas_call(
        write_out,
        out_shape=(
            pltpu.HBM(electric.shape, f32),
            pltpu.HBM(magnetic.shape, f32),
            pltpu.HBM((1, snaps), f32),
            pltpu.HBM((snaps,), f32),
        ),
        in_specs=[vmem] * 3,
        out_specs=(hbm,) * 4,
        scratch_shapes=[
            pltpu.SMEM((1, snaps), f32),
            pltpu.SMEM((snaps,), f32),
            pltpu.SemaphoreType.DMA((2, electric.shape[1] + 1)),
        ],
        compiler_params=pltpu.CompilerParams(vmem_limit_bytes=1024 * 1024),
    )(electric_end, magnetic_end, power)


def on_device(
    bloch_index,
    material,
    permittivity,
    absorption_peak,
    source_sheet,
    waveform,
    electric_in,
    magnetic_in,
):
    points = bloch_index.shape[0]
    results = [
        one_point(
            bloch_index[p : p + 1],
            material,
            permittivity,
            absorption_peak,
            source_sheet[p : p + 1],
            waveform,
            electric_in[p : p + 1],
            magnetic_in[p : p + 1],
        )
        for p in range(points)
    ]
    if points == 1:
        return results[0]
    electric_out, magnetic_out, reflected, mean = (list(r) for r in zip(*results))
    return (
        jnp.concatenate(electric_out, 0),
        jnp.concatenate(magnetic_out, 0),
        jnp.concatenate(reflected, 0),
        sum(mean) / points,
    )


def solution(mesh):
    in_specs = (
        P("ka", None),
        P("sp", None, None),
        P(),
        P(),
        P("ka", None, "sp", None),
        P(),
        P("ka", None, "sp", None, None),
        P("ka", None, "sp", None, None),
    )
    out_specs = (
        P("ka", None, "sp", None, None),
        P("ka", None, "sp", None, None),
        P("ka", None),
        P(),
    )
    return jax.shard_map(
        on_device, mesh=mesh, in_specs=in_specs, out_specs=out_specs, check_vma=False
    )
```

```python
import jax
import jax.numpy as jnp
from jax import lax
from jax.experimental import pallas as pl
from jax.experimental.pallas import tpu as pltpu
from jax.sharding import PartitionSpec as P

PML = 16
INTERVAL = 5
MPHASE = 64
NMAT = 3
TIME_STEP = 0.5
MESH = pl.DeviceIdType.MESH


def rotate(couple, cosine, sine):
    return (couple[0] * cosine - couple[1] * sine, couple[0] * sine + couple[1] * cosine)


def minus(left, right):
    return (left[0] - right[0], left[1] - right[1])


def plus(left, right):
    return (left[0] + right[0], left[1] + right[1])


def relax(couple, change, keep, gain):
    return tuple(keep * c + gain * d for c, d in zip(couple, change))


def kernel(
    bloch_in,
    perm_in,
    peak_in,
    wave_in,
    material_in,
    sheet_in,
    e_hbm,
    h_hbm,
    e_ref,
    h_ref,
    power_ref,
    bloch_ref,
    perm_ref,
    peak_ref,
    wave_ref,
    material_ref,
    sheet_ref,
    e_in,
    h_in,
    report_ref,
    got_report,
    keep_ref,
    gain_ref,
    drive_ref,
    out_e,
    out_w,
    got_e,
    got_w,
    tiny,
    got_tiny,
    ahead_ref,
    send_e,
    send_w,
    recv_e,
    recv_w,
    send_tiny,
    recv_tiny,
    load_sem,
    send_report,
    recv_report,
    entered,
):
    rows, width, depth = material_ref.shape
    steps = wave_ref.shape[0]
    slabs = lax.axis_size("sp")
    slab = lax.axis_index("sp")
    upper = lax.rem(slab + 1, slabs)
    lower = lax.rem(slab + slabs - 1, slabs)

    groups = lax.axis_size("ka")
    group = lax.axis_index("ka")
    everyone = groups * slabs
    me = group * slabs + slab

    def place(at):
        return {"ka": lax.div(at, slabs), "sp": lax.rem(at, slabs)}

    barrier = pltpu.get_barrier_semaphore()

    def greet(other):
        pl.semaphore_signal(barrier, inc=1, device_id=place(other), device_id_type=MESH)

    grid = groups % 4 == 0
    ahead_of = [("flip", 1), ("flip", 2)]
    stride = 1
    while stride < groups // 4 - 1:
        ahead_of.insert(0, ("line", 4 * stride))
        stride *= 2
    ahead_of = sorted(ahead_of[:-2], key=lambda turn: turn[1]) + ahead_of[-2:]
    stride = 1
    while stride < slabs // 2:
        ahead_of.append(("ring", stride))
        stride *= 2
    rounds = len(ahead_of) if grid else 0

    def peers(kind, stride):
        if kind == "flip":
            return [((group + stride * (1 - 2 * lax.rem(lax.div(group, stride), 2))) * slabs + slab, None)]
        if kind == "ring":
            return [
                (group * slabs + lax.rem(slab + stride, slabs), None),
                (group * slabs + lax.rem(slab + slabs - stride, slabs), None),
            ]
        return [
            ((group + stride) * slabs + slab, group + stride < groups),
            ((group - stride) * slabs + slab, group >= stride),
        ]

    def signal_to(semaphore, found):
        for other, exists in found:

            def signal():
                pl.semaphore_signal(
                    semaphore, inc=1, device_id=place(other), device_id_type=MESH
                )

            if exists is None:
                signal()
            else:
                pl.when(exists)(signal)

    def amount(found):
        return sum(1 if exists is None else exists.astype(jnp.int32) for _, exists in found)

    if grid:
        nearest = peers("ring", 1) + peers("flip", 1) + peers("flip", 2) + peers("line", 4)
        signal_to(barrier, nearest)
        greeted = amount(nearest)
    else:

        def greet_at(offset, carry):
            signal_to(barrier, [(lax.rem(me + offset, everyone), None)])
            return carry

        lax.fori_loop(1, everyone, greet_at, 0)
        greeted = everyone - 1

    def spread(turn):
        signal_to(entered.at[turn], peers(*ahead_of[turn]))

    def learn(turn):
        pl.semaphore_wait(entered.at[turn], amount(peers(*ahead_of[turn])))

    last_row = rows - 1
    loads = [
        pltpu.make_async_copy(src, dst, load_sem.at[at])
        for at, (src, dst) in enumerate(
            (
                (e_hbm.at[0, pl.ds(2, 4), 0], e_in.at[0, pl.ds(2, 4), 0]),
                (e_hbm.at[0, :, last_row], e_in.at[0, :, last_row]),
                (h_hbm.at[0, :, last_row], h_in.at[0, :, last_row]),
                (h_hbm.at[0, :, 0], h_in.at[0, :, 0]),
                (e_hbm.at[0, pl.ds(0, 2), 0], e_in.at[0, pl.ds(0, 2), 0]),
                (bloch_in, bloch_ref),
                (perm_in, perm_ref),
                (peak_in, peak_ref),
                (wave_in, wave_ref),
                (e_hbm.at[0, :, 1:last_row], e_in.at[0, :, 1:last_row]),
                (h_hbm.at[0, :, 1:last_row], h_in.at[0, :, 1:last_row]),
                (material_in, material_ref),
                (sheet_in, sheet_ref),
            )
        )
    ]
    for load in loads:
        load.start()

    def copy_e(slot, member):
        return pltpu.make_async_remote_copy(
            src_ref=out_e.at[slot, pl.ds(2 * member, 2)],
            dst_ref=got_e.at[slot, pl.ds(2 * member, 2)],
            send_sem=send_e.at[slot, member],
            recv_sem=recv_e.at[slot, member],
            device_id={"sp": lower},
            device_id_type=MESH,
        )

    loads[0].wait()
    for member in range(4):
        out_e[0, member] = e_in[0, 2 + member, 0].astype(jnp.float32)
    pl.semaphore_wait(barrier, greeted)
    copy_e(0, 0).start()
    copy_e(0, 1).start()
    for load in loads[5:9]:
        load.wait()

    height = lax.broadcasted_iota(jnp.int32, (8, depth), 1).astype(jnp.float32)
    low_depth = jnp.maximum(PML - height, 0.0) / PML
    high_depth = jnp.maximum(height - (depth - 1 - PML), 0.0) / PML
    conduct = peak_ref[0] * (
        low_depth * low_depth * low_depth + high_depth * high_depth * high_depth
    )
    half_mag = conduct * (0.5 * TIME_STEP)
    h_keep = ((1.0 - half_mag) / (1.0 + half_mag))[0:1]
    h_gain = (-TIME_STEP / (1.0 + half_mag))[0:1]
    tables = []
    for level in range(NMAT):
        relative = jnp.full((8, depth), perm_ref[level], jnp.float32)
        half_ele = conduct * (0.5 * TIME_STEP) / relative
        tables.append(
            (
                ((1.0 - half_ele) / (1.0 + half_ele))[0:1],
                (TIME_STEP / relative / (1.0 + half_ele))[0:1],
            )
        )

    def trig(member):
        angle = jnp.full((8, depth), bloch_ref[0, member], jnp.int32).astype(jnp.float32)
        angle = 2.0 * jnp.pi * angle / MPHASE
        return jnp.cos(angle)[0:1], jnp.sin(angle)[0:1]

    cos_x, sin_x = trig(0)
    cos_y, sin_y = trig(1)
    at_end = (slab == slabs - 1).astype(jnp.float32)
    at_start = (slab == 0).astype(jnp.float32)
    end_cos = at_end * cos_x + (1.0 - at_end)
    end_sin = at_end * sin_x
    start_cos = at_start * cos_x + (1.0 - at_start)
    start_sin = -at_start * sin_x

    lane = lax.broadcasted_iota(jnp.int32, (width, depth), 1)
    last_lane = lane == depth - 1
    first_lane = lane == 0
    sub = lax.broadcasted_iota(jnp.int32, (8, depth), 0)

    def above_z(couple):
        return tuple(jnp.where(last_lane, 0.0, pltpu.roll(v, depth - 1, 1)) for v in couple)

    def below_z(couple):
        return tuple(jnp.where(first_lane, 0.0, pltpu.roll(v, 1, 1)) for v in couple)

    def above_y(couple):
        moved = tuple(pltpu.roll(v, width - 1, 0) for v in couple)
        tail = tuple(v[width - 8 :] for v in moved)
        turned = rotate(tail, cos_y, sin_y)
        return tuple(
            jnp.concatenate([v[: width - 8], jnp.where(sub == 7, r, w)], axis=0)
            for v, r, w in zip(moved, turned, tail)
        )

    def below_y(couple):
        moved = tuple(pltpu.roll(v, 1, 0) for v in couple)
        head = tuple(v[:8] for v in moved)
        turned = rotate(head, cos_y, -sin_y)
        return tuple(
            jnp.concatenate([jnp.where(sub == 0, r, w), v[8:]], axis=0)
            for v, r, w in zip(moved, turned, head)
        )

    def get(ref, member, x):
        return (ref[0, 2 * member, x], ref[0, 2 * member + 1, x])

    def put(ref, member, x, couple):
        ref[0, 2 * member, x] = couple[0]
        ref[0, 2 * member + 1, x] = couple[1]

    def get_plane(ref, slot, member):
        return (ref[slot, 2 * member], ref[slot, 2 * member + 1])

    def put_plane(ref, slot, member, couple):
        ref[slot, 2 * member] = couple[0]
        ref[slot, 2 * member + 1] = couple[1]

    def new_hx(x, ey, ez):
        change = minus(minus(above_y(ez), ez), minus(above_z(ey), ey))
        return relax(get(h_ref, 0, x), change, h_keep, h_gain)

    def new_hy(x, ex, ez, ez_next):
        change = minus(minus(above_z(ex), ex), minus(ez_next, ez))
        return relax(get(h_ref, 1, x), change, h_keep, h_gain)

    def new_hz(x, ex, ey, ey_next):
        change = minus(minus(ey_next, ey), minus(above_y(ex), ex))
        return relax(get(h_ref, 2, x), change, h_keep, h_gain)

    def hx_plane(x):
        put(h_ref, 0, x, new_hx(x, get(e_ref, 1, x), get(e_ref, 2, x)))

    def h_plane(x):
        ex, ey, ez = get(e_ref, 0, x), get(e_ref, 1, x), get(e_ref, 2, x)
        put(h_ref, 0, x, new_hx(x, ey, ez))
        put(h_ref, 1, x, new_hy(x, ex, ez, get(e_ref, 2, x + 1)))
        put(h_ref, 2, x, new_hz(x, ex, ey, get(e_ref, 1, x + 1)))

    def part_y(ex, ez, hy):
        return relax(hy, plus(minus(above_z(ex), ex), ez), h_keep, h_gain)

    def part_z(ex, ey, hz):
        return relax(hz, minus(minus(ex, above_y(ex)), ey), h_keep, h_gain)

    def partial_y(slot):
        x = rows - 1
        put_plane(out_w, slot, 0, part_y(get(e_ref, 0, x), get(e_ref, 2, x), get(h_ref, 1, x)))

    def partial_z(slot):
        x = rows - 1
        put_plane(out_w, slot, 1, part_z(get(e_ref, 0, x), get(e_ref, 1, x), get(h_ref, 2, x)))

    def whole_hz(slot, beyond_y):
        beyond_y = rotate(beyond_y, end_cos, end_sin)
        return tuple(w + h_gain * b for w, b in zip(get_plane(out_w, slot, 1), beyond_y))

    def whole_hy(slot, beyond_z):
        beyond_z = rotate(beyond_z, end_cos, end_sin)
        return tuple(w - h_gain * b for w, b in zip(get_plane(out_w, slot, 0), beyond_z))

    def hz_below(w_z, ey):
        turned = rotate(w_z, start_cos, start_sin)
        return tuple(w + h_gain * e for w, e in zip(turned, ey))

    def hy_below(w_y, ez):
        turned = rotate(w_y, start_cos, start_sin)
        return tuple(w - h_gain * e for w, e in zip(turned, ez))

    def new_ex(x, drive, hy, hz):
        change = minus(minus(hz, below_y(hz)), minus(hy, below_z(hy)))
        change = (change[0] - drive * drive_ref[0, x], change[1] - drive * drive_ref[1, x])
        return relax(get(e_ref, 0, x), change, keep_ref[x], gain_ref[x])

    def new_ey(x, ey, hx, hz, hz_prev):
        change = minus(minus(hx, below_z(hx)), minus(hz, hz_prev))
        return relax(ey, change, keep_ref[x], gain_ref[x])

    def new_ez(x, hx, hy, hy_prev):
        change = minus(minus(hy, hy_prev), minus(hx, below_y(hx)))
        return relax(get(e_ref, 2, x), change, keep_ref[x], gain_ref[x])

    def e_update(x, drive, hy_prev, hz_prev):
        hx, hy, hz = get(h_ref, 0, x), get(h_ref, 1, x), get(h_ref, 2, x)
        put(e_ref, 0, x, new_ex(x, drive, hy, hz))
        ey = new_ey(x, get(e_ref, 1, x), hx, hz, hz_prev)
        put(e_ref, 1, x, ey)
        ez = new_ez(x, hx, hy, hy_prev)
        put(e_ref, 2, x, ez)
        return ey, ez

    def e_middle(x, drive):
        return e_update(x, drive, get(h_ref, 1, x - 1), get(h_ref, 2, x - 1))

    def copy_w(slot, member):
        return pltpu.make_async_remote_copy(
            src_ref=out_w.at[slot, pl.ds(2 * member, 2)],
            dst_ref=got_w.at[slot, pl.ds(2 * member, 2)],
            send_sem=send_w.at[slot, member],
            recv_sem=recv_w.at[slot, member],
            device_id={"sp": upper},
            device_id_type=MESH,
        )

    square = lax.broadcasted_iota(jnp.int32, (width, width), 0) == lax.broadcasted_iota(
        jnp.int32, (width, width), 1
    )
    monitor = PML + 6
    band = monitor // 8 * 8

    def copy_tiny(at, other):
        return pltpu.make_async_remote_copy(
            src_ref=tiny.at[at],
            dst_ref=got_tiny.at[at],
            send_sem=send_tiny.at[at],
            recv_sem=recv_tiny.at[at],
            device_id={"sp": other},
            device_id_type=MESH,
        )

    def pack(at, member, couple):
        tiny[at, member] = jnp.concatenate(couple, axis=0).T[band : band + 8]

    def unpack(at, member):
        before = jnp.zeros((band, 2 * width), jnp.float32)
        after = jnp.zeros((depth - band - 8, 2 * width), jnp.float32)
        tall = jnp.concatenate([before, got_tiny[at, member], after], axis=0).T
        return tall[:width], tall[width:]

    ahead_e1, ahead_e2, ahead_e3 = (copy_tiny(at, lower) for at in range(3))
    ahead_w2, ahead_w3 = (copy_tiny(at, upper) for at in range(3, 5))

    def widen(x, carry):
        for member in range(6):
            e_ref[0, member, x] = e_in[0, member, x].astype(jnp.float32)
            h_ref[0, member, x] = h_in[0, member, x].astype(jnp.float32)
        return carry

    for load in loads[1:5]:
        load.wait()
    widen(rows - 1, 0)
    partial_z(0)
    copy_w(0, 1).start()
    partial_y(0)
    copy_w(0, 0).start()
    widen(0, 0)
    for load in loads[9:]:
        load.wait()
    lax.fori_loop(1, rows - 1, widen, 0)

    report_ref[...] = jnp.zeros_like(report_ref)

    def prepare(x, carry):
        kind = material_ref[x]
        keep, gain = tables[0]
        for level in range(1, NMAT):
            keep = jnp.where(kind == level, tables[level][0], keep)
            gain = jnp.where(kind == level, tables[level][1], gain)
        keep_ref[x] = keep
        gain_ref[x] = gain
        for part in range(2):
            row = sheet_ref[0, part, pl.ds(x, 1), :]
            column = jnp.sum(jnp.where(square, row, 0.0), axis=1, keepdims=True)
            drive_ref[part, x] = jnp.where(lane == PML + 2, column, 0.0)
        return carry

    together = 4 if rows % 4 == 0 else 1

    def prepare_some(group_of, carry):
        for at in range(together):
            prepare(group_of * together + at, carry)
        return carry

    lax.fori_loop(0, rows // together, prepare_some, 0)

    def power(x, total):
        for member in range(4):
            value = e_ref[0, member, x]
            total = total + value * value
        return total

    row_lane = lax.broadcasted_iota(jnp.int32, (1, depth), 1)
    empty = jnp.zeros((width, depth), jnp.float32)
    assert steps % (2 * INTERVAL) == 0 and rows > 6

    def note(total, at):
        amount = jnp.sum(jnp.where(lane == monitor, total, 0.0), axis=0, keepdims=True)
        amount = jnp.sum(amount, axis=1, keepdims=True)
        report_ref[...] += jnp.where(row_lane == at, amount, 0.0)

    def first_y(slot, later, sent, go):
        copy_w(slot, 1).wait_recv()
        ey = get(e_ref, 1, 0)
        hz_prev = hz_below(get_plane(got_w, slot, 1), ey)
        ey = new_ey(0, ey, get(h_ref, 0, 0), get(h_ref, 2, 0), hz_prev)
        put(e_ref, 1, 0, ey)
        if go:
            pl.when(sent)(lambda: copy_e(later, 0).wait_send())
            put_plane(out_e, later, 0, ey)
            copy_e(later, 0).start()

    def first_z(slot, later, sent, go):
        copy_w(slot, 0).wait_recv()
        hy_prev = hy_below(get_plane(got_w, slot, 0), get(e_ref, 2, 0))
        ez = new_ez(0, get(h_ref, 0, 0), get(h_ref, 1, 0), hy_prev)
        put(e_ref, 2, 0, ez)
        if go:
            pl.when(sent)(lambda: copy_e(later, 1).wait_send())
            put_plane(out_e, later, 1, ez)
            copy_e(later, 1).start()

    def first_yz_ahead(slot, later, at, copy):
        first_y(slot, later, True, False)
        first_z(slot, later, True, False)
        send_columns(at, copy)
        for member in range(2):
            copy_e(later, member).wait_send()
            put_plane(out_e, later, member, get(e_ref, 1 + member, 0))
            copy_e(later, member).start()

    def send_columns(at, copy):
        pack(at, 0, get(e_ref, 1, 0))
        pack(at, 1, get(e_ref, 2, 0))
        copy.start()

    def first_x(drive):
        put(e_ref, 0, 0, new_ex(0, drive, get(h_ref, 1, 0), get(h_ref, 2, 0)))

    def end_fields(slot, drive):
        x = rows - 1
        copy_e(slot, 0).wait_recv()
        hz = whole_hz(slot, get_plane(got_e, slot, 0))
        put(h_ref, 2, x, hz)
        hx = get(h_ref, 0, x)
        put(e_ref, 1, x, new_ey(x, get(e_ref, 1, x), hx, hz, get(h_ref, 2, x - 1)))
        copy_e(slot, 1).wait_recv()
        hy = whole_hy(slot, get_plane(got_e, slot, 1))
        put(h_ref, 1, x, hy)
        put(e_ref, 0, x, new_ex(x, drive, hy, get(h_ref, 2, x)))
        put(e_ref, 2, x, new_ez(x, get(h_ref, 0, x), hy, get(h_ref, 1, x - 1)))

    def give_w(later):
        copy_w(later, 1).wait_send()
        copy_w(later, 0).wait_send()
        partial_z(later)
        copy_w(later, 1).start()
        partial_y(later)
        copy_w(later, 0).start()

    def sides(t, slot, later, drive):
        def left():
            first_x(drive)
            ahead = t == steps - 4

            @pl.when(ahead)
            def _():
                first_yz_ahead(slot, later, 0, ahead_e1)

            @pl.when(jnp.logical_not(ahead))
            def _():
                first_y(slot, later, t >= 1, True)
                first_z(slot, later, t >= 1, True)

        def right():
            end_fields(slot, drive)

            @pl.when(t >= 1)
            def _():
                copy_w(later, 1).wait_send()
                copy_w(later, 0).wait_send()

            partial_z(later)
            copy_w(later, 1).start()
            partial_y(later)
            copy_w(later, 0).start()

        return left, right

    def before_sides():
        h_plane(0)
        h_plane(1)
        h_plane(rows - 2)
        hx_plane(rows - 1)

    def between_sides(drive):
        def both(x, held):
            e_middle(x, drive)
            h_plane(x + 1)
            return held

        lax.fori_loop(1, rows - 3, both, 0)
        e_middle(rows - 3, drive)
        e_middle(rows - 2, drive)

    def step(t, carry):
        slot = lax.rem(t, 2)
        later = lax.rem(t + 1, 2)
        drive = wave_ref[t]
        even = slot == 0
        left, right = sides(t, slot, later, drive)

        for turn in range(min(rounds, steps - 3)):

            @pl.when(t == turn)
            def _():
                if turn > 0:
                    learn(turn - 1)
                spread(turn)

        before_sides()
        pl.when(even)(right)
        pl.when(jnp.logical_not(even))(left)
        between_sides(drive)
        pl.when(even)(left)
        pl.when(jnp.logical_not(even))(right)

        @pl.when(lax.rem(t + 1, INTERVAL) == 0)
        def _():
            note(lax.fori_loop(0, rows, power, empty), lax.div(t, INTERVAL))

        return carry

    lax.fori_loop(0, steps - 3, step, 0)
    for turn in range(min(rounds, steps - 3), rounds):
        if turn > 0:
            learn(turn - 1)
        spread(turn)
    if rounds > 0:
        learn(rounds - 1)

    def tell(offset):
        return pltpu.make_async_remote_copy(
            src_ref=report_ref,
            dst_ref=got_report.at[me],
            send_sem=send_report,
            recv_sem=recv_report,
            device_id=place(lax.rem(me + offset, everyone)),
            device_id_type=MESH,
        )

    def tell_start(offset, carry):
        tell(offset).start()
        return carry

    end = rows - 1
    one, two, three = ((steps - 3 + at) % 2 for at in range(3))
    drive_one, drive, last_drive = (wave_ref[steps - 3 + at] for at in range(3))
    before_sides()
    between_sides(drive_one)
    ahead_e1.wait_recv()
    hz = whole_hz(one, unpack(0, 0))
    hy = whole_hy(one, unpack(0, 1))
    hx, hy_prev, hz_prev = get(h_ref, 0, end), get(h_ref, 1, end - 1), get(h_ref, 2, end - 1)
    ex = new_ex(end, drive_one, hy, hz)
    pack(3, 1, part_z(ex, new_ey(end, get(e_ref, 1, end), hx, hz, hz_prev), hz))
    pack(3, 0, part_y(ex, new_ez(end, hx, hy, hy_prev), hy))
    ahead_w2.start()

    first_x(drive_one)
    first_yz_ahead(one, two, 1, ahead_e2)

    h_plane(0)
    h_plane(1)

    def both(x, held):
        e_middle(x, drive)
        h_plane(x + 1)
        return held

    lax.fori_loop(1, end - 2, both, 0)
    e_middle(end - 2, drive)
    end_fields(one, drive_one)
    copy_w(two, 1).wait_send()
    copy_w(two, 0).wait_send()
    partial_z(two)
    copy_w(two, 1).start()
    partial_y(two)
    h_plane(end - 1)
    hx_plane(end)

    ahead_e2.wait_recv()
    hz = whole_hz(two, unpack(1, 0))
    hy = whole_hy(two, unpack(1, 1))
    ex = new_ex(end, drive, hy, hz)
    ey = new_ey(end, get(e_ref, 1, end), get(h_ref, 0, end), hz, get(h_ref, 2, end - 1))
    w_z = part_z(ex, ey, hz)
    pack(4, 0, w_z)
    pack(4, 1, w_z)
    ahead_w3.start()

    first_x(drive)
    ahead_w2.wait_recv()
    ey, ez = get(e_ref, 1, 0), get(e_ref, 2, 0)
    hy_prev, hz_prev = hy_below(unpack(3, 0), ez), hz_below(unpack(3, 1), ey)
    ey = new_ey(0, ey, get(h_ref, 0, 0), get(h_ref, 2, 0), hz_prev)
    ez = new_ez(0, get(h_ref, 0, 0), get(h_ref, 1, 0), hy_prev)
    put_plane(ahead_ref, 0, 0, ey)
    put_plane(ahead_ref, 0, 1, ez)
    pack(2, 0, ey)
    pack(2, 1, ez)
    ahead_e3.start()
    copy_w(two, 0).start()
    e_middle(end - 1, drive)

    h_plane(1)
    h_plane(2)

    def both_power(x, total):
        e_middle(x, last_drive)
        h_plane(x + 1)
        return power(x, total)

    total = lax.fori_loop(2, end - 2, both_power, empty)
    e_middle(end - 2, last_drive)
    total = power(end - 2, total)

    end_fields(two, drive)
    give_w(three)
    h_plane(end - 1)
    hx_plane(end)
    e_middle(end - 1, last_drive)
    total = power(end - 1, total)

    ex, ey, ez = get(e_ref, 0, 0), get_plane(ahead_ref, 0, 0), get_plane(ahead_ref, 0, 1)
    hx = new_hx(0, ey, ez)
    hy = new_hy(0, ex, ez, get(e_ref, 2, 1))
    hz = new_hz(0, ex, ey, get(e_ref, 1, 1))
    hx1, hy1, hz1 = get(h_ref, 0, 1), get(h_ref, 1, 1), get(h_ref, 2, 1)
    ahead_w3.wait_recv()
    hz_prev = hz_below(unpack(4, 1), ey)
    for value in (
        new_ex(0, last_drive, hy, hz)
        + new_ey(0, ey, hx, hz, hz_prev)
        + new_ex(1, last_drive, hy1, hz1)
        + new_ey(1, get(e_ref, 1, 1), hx1, hz1, hz)
    ):
        total = total + value * value
    ahead_e3.wait_recv()
    hx = get(h_ref, 0, end)
    hz = whole_hz(three, unpack(2, 0))
    hy = whole_hy(three, unpack(2, 1))
    for value in new_ex(end, last_drive, hy, hz) + new_ey(
        end, get(e_ref, 1, end), hx, hz, get(h_ref, 2, end - 1)
    ):
        total = total + value * value
    note(total, steps // INTERVAL - 1)
    lax.fori_loop(1, everyone, tell_start, 0)
    got_report[me] = report_ref[...]

    first_y(two, three, True, True)
    first_z(two, three, True, True)

    h_plane(0)
    e_middle(1, last_drive)
    first_x(last_drive)
    first_y(three, two, False, False)
    first_z(three, two, False, False)
    end_fields(three, last_drive)
    for at in range(2):
        for member in range(2):
            copy_e(at, member).wait_send()
            copy_w(at, member).wait_send()
    for copy in (ahead_e1, ahead_e2, ahead_e3, ahead_w2, ahead_w3):
        copy.wait_send()
    everything = got_report.at[pl.ds(0, everyone - 1)]
    pltpu.make_async_copy(everything, everything, recv_report).wait()
    pltpu.make_async_copy(everything, everything, send_report).wait()

    def gather(at, held):
        return held + got_report[group * slabs + at]

    ours = lax.fori_loop(0, slabs, gather, jnp.zeros((1, depth), jnp.float32))
    total = jnp.sum(got_report[...], axis=0)
    cells = rows * slabs * width
    power_ref[0:1] = ours / cells
    power_ref[1:2] = total / cells / groups


def write_out(e_ref, h_ref, power_ref, e_out, h_out, reflected_out, mean_out, own, mean, sems):
    members = e_ref.shape[1]
    snaps = mean.shape[0]
    writes = [
        pltpu.make_async_copy(src.at[0, member], dst.at[0, member], sems.at[at, member])
        for at, (src, dst) in enumerate(((e_ref, e_out), (h_ref, h_out)))
        for member in range(members)
    ]
    for write in writes:
        write.start()
    lane = lax.broadcasted_iota(jnp.int32, (1, power_ref.shape[1]), 1)
    for at in range(snaps):
        own[0, at] = jnp.sum(jnp.where(lane == at, power_ref[0:1], 0.0))
        mean[at] = jnp.sum(jnp.where(lane == at, power_ref[1:2], 0.0))
    small = [
        pltpu.make_async_copy(own, reflected_out, sems.at[0, members]),
        pltpu.make_async_copy(mean, mean_out, sems.at[1, members]),
    ]
    for write in small:
        write.start()
    for write in writes + small:
        write.wait()


def one_point(bloch, material, permittivity, peak, sheet, waveform, electric, magnetic):
    rows, width, depth = material.shape
    snaps = waveform.shape[0] // INTERVAL
    everyone = lax.axis_size("ka") * lax.axis_size("sp")
    hbm = pl.BlockSpec(memory_space=pltpu.HBM)
    vmem = pl.BlockSpec(memory_space=pltpu.VMEM)
    plane = (2, 4, width, depth)
    f32 = jnp.float32
    electric_end, magnetic_end, power = pl.pallas_call(
        kernel,
        out_shape=(
            jax.ShapeDtypeStruct(electric.shape, f32),
            jax.ShapeDtypeStruct(magnetic.shape, f32),
            jax.ShapeDtypeStruct((8, depth), f32),
        ),
        in_specs=[hbm] * 8,
        out_specs=(vmem, vmem, vmem),
        scratch_shapes=[
            pltpu.SMEM(bloch.shape, jnp.int32),
            pltpu.SMEM(permittivity.shape, f32),
            pltpu.SMEM(peak.shape, f32),
            pltpu.SMEM(waveform.shape, f32),
            pltpu.VMEM(material.shape, jnp.int32),
            pltpu.VMEM(sheet.shape, f32),
            pltpu.VMEM(electric.shape, electric.dtype),
            pltpu.VMEM(magnetic.shape, magnetic.dtype),
            pltpu.VMEM((1, depth), f32),
            pltpu.VMEM((everyone, 1, depth), f32),
            pltpu.VMEM((rows, width, depth), f32),
            pltpu.VMEM((rows, width, depth), f32),
            pltpu.VMEM((2, rows, width, depth), f32),
            pltpu.VMEM(plane, f32),
            pltpu.VMEM(plane, f32),
            pltpu.VMEM(plane, f32),
            pltpu.VMEM(plane, f32),
            pltpu.VMEM((5, 2, 8, 2 * width), f32),
            pltpu.VMEM((5, 2, 8, 2 * width), f32),
            pltpu.VMEM((1, 4, width, depth), f32),
            pltpu.SemaphoreType.DMA((2, 2)),
            pltpu.SemaphoreType.DMA((2, 2)),
            pltpu.SemaphoreType.DMA((2, 2)),
            pltpu.SemaphoreType.DMA((2, 2)),
            pltpu.SemaphoreType.DMA((5,)),
            pltpu.SemaphoreType.DMA((5,)),
            pltpu.SemaphoreType.DMA((13,)),
            pltpu.SemaphoreType.DMA,
            pltpu.SemaphoreType.DMA,
            pltpu.SemaphoreType.REGULAR((2 + everyone.bit_length(),)),
        ],
        compiler_params=pltpu.CompilerParams(
            collective_id=0, has_side_effects=True, vmem_limit_bytes=40 * 1024 * 1024
        ),
    )(*((v if v.shape == (1,) else pltpu.with_memory_space_constraint(v, pltpu.HBM)) for v in (bloch, permittivity, peak, waveform, material, sheet, electric, magnetic)))
    return pl.pallas_call(
        write_out,
        out_shape=(
            pltpu.HBM(electric.shape, f32),
            pltpu.HBM(magnetic.shape, f32),
            pltpu.HBM((1, snaps), f32),
            pltpu.HBM((snaps,), f32),
        ),
        in_specs=[vmem] * 3,
        out_specs=(hbm,) * 4,
        scratch_shapes=[
            pltpu.SMEM((1, snaps), f32),
            pltpu.SMEM((snaps,), f32),
            pltpu.SemaphoreType.DMA((2, electric.shape[1] + 1)),
        ],
        compiler_params=pltpu.CompilerParams(vmem_limit_bytes=1024 * 1024),
    )(electric_end, magnetic_end, power)


def on_device(
    bloch_index,
    material,
    permittivity,
    absorption_peak,
    source_sheet,
    waveform,
    electric_in,
    magnetic_in,
):
    points = bloch_index.shape[0]
    results = [
        one_point(
            bloch_index[p : p + 1],
            material,
            permittivity,
            absorption_peak,
            source_sheet[p : p + 1],
            waveform,
            electric_in[p : p + 1],
            magnetic_in[p : p + 1],
        )
        for p in range(points)
    ]
    if points == 1:
        return results[0]
    electric_out, magnetic_out, reflected, mean = (list(r) for r in zip(*results))
    return (
        jnp.concatenate(electric_out, 0),
        jnp.concatenate(magnetic_out, 0),
        jnp.concatenate(reflected, 0),
        sum(mean) / points,
    )


def solution(mesh):
    in_specs = (
        P("ka", None),
        P("sp", None, None),
        P(),
        P(),
        P("ka", None, "sp", None),
        P(),
        P("ka", None, "sp", None, None),
        P("ka", None, "sp", None, None),
    )
    out_specs = (
        P("ka", None, "sp", None, None),
        P("ka", None, "sp", None, None),
        P("ka", None),
        P(),
    )
    return jax.shard_map(
        on_device, mesh=mesh, in_specs=in_specs, out_specs=out_specs, check_vma=False
    )
```
